256 devices in a mesh: row: 4 (over x), col: 8 (over z), depth: 8 (over y, core).
Axes of the slice: x: 4, y: 4, z: 8, core: 2. Of those that a mesh axis runs over, the one named last changes fastest.
Arguments:
- trailing: float32 [1504, 48128], P('depth', ('row', 'col')), may hold values from -6 to 6
- panel_block: float32 [48128, 1024], P(('row', 'col', 'depth')), may hold values from -6 to 6
- factor_panel: float32 [48128, 1024], P(('row', 'col', 'depth')), may hold values from -0.1875 to 0.1875
- corner_block: float32 [1024, 1024], P(('row', 'col', 'depth')), may hold values from -6 to 6, as said below
- corner_inverse: float32 [1024, 1024], P(('row', 'col', 'depth')), may hold values from -1 to 2, as said below
Outputs:
- trailing_out: float32 [1504, 48128], P('depth', ('row', 'col'))
- panel_out: float32 [48128, 1024], P(('row', 'col', 'depth'))
- corner_out: float32 [1024, 1024], P(('row', 'col', 'depth'))
The draws below stay inside these ranges and needn't reach their ends.
Inputs may be any that keep to these rules, and one draw needn't show every extreme that they name: `corner_block`: symmetric. `corner_inverse`: lower triangular, diagonal between 1 and 2.
All inputs are finite; a program needn't handle non-finite values.
Results may differ from the reference program's by a relative error of at most 0.00012.
Values sent between devices are 32-bit elements; how exact they have to be, the bound alone decides.
A program may use at most 128 MiB of HBM per device.

```python
import jax
import jax.numpy as jnp
from jax import lax

NB = 1024
M = 48128
SPAN = 1
SLAB = 1504
N_DEPTH = 8


def draw_corner_block(key, part):
    noise = jax.random.truncated_normal(jax.random.fold_in(key, 11), -4.0, 4.0, (NB, NB), jnp.float32)
    return (noise + noise.T) * 0.7071


def draw_corner_inverse(key, part):
    below = jax.random.truncated_normal(jax.random.fold_in(key, 23), -4.0, 4.0, (NB, NB), jnp.float32)
    diagonal = jax.random.uniform(jax.random.fold_in(key, 29), (NB,), jnp.float32, 1.0, 2.0)
    strict = jnp.tril(below, -1) * (0.5 / NB ** 0.5)
    return strict + jnp.diag(diagonal)


def block_scale(rng, shape, cuts, least, largest):
    level = 1.0
    for position, shards_of in cuts:
        draws = jax.random.uniform(jax.random.fold_in(jax.random.fold_in(rng, 6), position), (shards_of,), jnp.float32, least / len(cuts), largest / len(cuts))
        level = level * jnp.repeat(jnp.exp(draws), shape[position] // shards_of).reshape((-1,) + (1,) * (len(shape) - 1 - position))
    return level


def gaussian(stream_key, shape, scale, limit, cuts=(), dtype=jnp.bfloat16):
    loudness = block_scale(stream_key, shape, cuts, -0.22, 0.18) if cuts else 1.0
    array = jax.random.normal(stream_key, shape, jnp.float32) * scale * loudness
    return jnp.minimum(jnp.maximum(array, -limit), limit).astype(dtype)


def setup_inputs(seed: int = 0) -> dict:
    arg_keys = jax.random.split(jax.random.key(seed), 6)
    trailing = gaussian(arg_keys[0], (SLAB, M), 1.0, 6.0, ((0, 8), (1, 32)), jnp.float32)
    panel_block = gaussian(arg_keys[1], (M, NB), 1.0, 6.0, ((0, 256),), jnp.float32)
    factor_panel = gaussian(arg_keys[2], (M, NB), NB ** -0.5, 0.1875, ((0, 256),), jnp.float32)
    corner_block = draw_corner_block(jax.random.fold_in(arg_keys[5], 71), 0)
    corner_inverse = draw_corner_inverse(jax.random.fold_in(arg_keys[5], 71), 0)
    return dict(trailing=trailing, panel_block=panel_block, factor_panel=factor_panel, corner_block=corner_block, corner_inverse=corner_inverse)


def matmul(left, right):
    return jnp.dot(left, right, precision=lax.Precision.HIGHEST, preferred_element_type=jnp.float32)


def permute(matrix):
    block = matrix[:SLAB]
    shaped = block.reshape(SPAN, N_DEPTH, SLAB // (SPAN * N_DEPTH), block.shape[1])
    return jnp.transpose(shaped, (1, 0, 2, 3)).reshape(SLAB, block.shape[1])


def reference(trailing, panel_block, factor_panel, corner_block, corner_inverse):
    corner_out = matmul(corner_inverse, matmul(corner_block, corner_inverse.T))
    scaled = matmul(panel_block, corner_inverse.T)
    coupling = matmul(factor_panel, corner_out)
    half_panel = scaled - 0.5 * coupling
    panel_out = half_panel - 0.5 * coupling
    update = matmul(permute(half_panel), factor_panel.T) + matmul(permute(factor_panel), half_panel.T)
    trailing_out = trailing - update
    return trailing_out, panel_out, corner_out
```

```python
import functools

import jax
import jax.numpy as jnp
from jax import lax
from jax.experimental import pallas as pl
from jax.experimental.pallas import tpu as pltpu
from jax.sharding import PartitionSpec as P

F32, BF16 = jnp.float32, jnp.bfloat16
MESH = pl.DeviceIdType.MESH
NN = (((1,), (0,)), ((), ()))
NT = (((1,), (1,)), ((), ()))


def split(x):
    hi = x.astype(BF16)
    return hi, (x - hi.astype(F32)).astype(BF16)


def dot(a, b, dims):
    return lax.dot_general(a, b, dims, preferred_element_type=F32)


def dot3(ah, al, bh, bl, dims):
    return dot(ah, bh, dims) + dot(ah, bl, dims) + dot(al, bh, dims)


class Ring:
    def __init__(self, n, me, axis, block, send, recv):
        self.n, self.me, self.axis, self.block = n, me, axis, block
        self.send, self.recv, self.steps = send, recv, n // 2

    def has(self, way, step, chunk):
        return step < self.steps or chunk == way

    def index(self, way, step, chunk):
        return (way * self.steps + step - 1) * 2 + chunk

    def copy(self, way, step, chunk, incoming=False):
        sign = 1 if way == 0 else -1
        hops = step if incoming else step - 1
        origin = lax.rem(self.me - sign * hops + self.n, self.n)
        target = lax.rem(self.me + sign + self.n, self.n)
        ref = self.block(origin, chunk)
        k = self.index(way, step, chunk)
        return pltpu.make_async_remote_copy(
            src_ref=ref, dst_ref=ref, send_sem=self.send.at[k], recv_sem=self.recv.at[k],
            device_id={self.axis: target}, device_id_type=MESH,
        )

    def order(self, step):
        keys = []
        for at in range(2):
            for way in range(2):
                chunk = at if way == 0 else 1 - at
                if self.has(way, step, chunk):
                    keys.append((way, step, chunk))
        return keys

    def start(self, step):
        for key in self.order(step):
            self.copy(*key).start()

    def arrived(self, way, step, chunk):
        self.copy(way, step, chunk, incoming=True).wait_recv()

    def forward(self, way, step, chunk):
        if step < self.steps and self.has(way, step + 1, chunk):
            self.copy(way, step + 1, chunk).start()

    def take(self, step, then=None):
        for key in self.order(step):
            self.arrived(*key)
            self.forward(*key)
            if then is not None:
                then(*key)

    def run(self):
        self.start(1)
        for step in range(1, self.steps + 1):
            self.take(step)

    def drain(self):
        for step in range(1, self.steps + 1):
            for key in self.order(step):
                self.copy(*key).wait_send()


def kernel(
    dims, trailing, a_in, f_in, s_in, w_in, t_out, p_out, c_out,
    rbuf, rhi, rlo, lsrc, lbuf, lhi, llo, mbuf, rows4, swap, whi, wlo, shi, slo, chi, clo,
    yhi, ylo, cblk, pq_hi, pq_lo, pbuf, ubuf, tbuf, cbuf,
    load, ysend, yrecv, rsend, rrecv, ms_send, ms_recv, mb_send, mb_recv, ls_send, ls_recv,
    lb_send, lb_recv, dr_send, dr_recv, dm_send, dm_recv, sw_send, sw_recv, sc_send, sc_recv,
):
    nx, nz, ny = dims
    nd = 2 * ny
    rows, width = a_in.shape
    whole = rows // 8 * 8
    x, z, depth = lax.axis_index("row"), lax.axis_index("col"), lax.axis_index("depth")
    y, core = depth // 2, lax.rem(depth, 2)
    lx, lz = lbuf.shape[1] // nx, width // nz
    half = width // 2
    other = y * 2 + 1 - core
    root = jnp.logical_and(x == 0, z == 0)

    def cols(chunk):
        return pl.ds(chunk * half, half)

    def remote(src, dst, send, recv, device):
        return pltpu.make_async_remote_copy(
            src_ref=src, dst_ref=dst, send_sem=send, recv_sem=recv, device_id=device, device_id_type=MESH
        )

    loads = [
        (w_in, rows4.at[0]),
        (s_in, rows4.at[1]),
        (a_in, rbuf.at[depth, 0]),
        (f_in, rbuf.at[depth, 1]),
        (a_in.at[pl.ds(0, whole)], lsrc.at[0, pl.ds(0, whole)]),
        (f_in.at[pl.ds(0, whole)], lsrc.at[1, pl.ds(0, whole)]),
        (trailing, tbuf),
    ]
    local = [pltpu.make_async_copy(src, dst, load.at[i]) for i, (src, dst) in enumerate(loads)]
    for copy in local:
        copy.start()

    barrier = pltpu.get_barrier_semaphore()
    peers = [{"depth": other}]
    peers += [{"depth": lax.rem(y + j, ny) * 2 + core} for j in range(1, ny)]
    peers += [{"col": lax.rem(z + 1, nz)}, {"col": lax.rem(z + nz - 1, nz)}]
    peers += [{"row": lax.rem(x + 1, nx)}, {"row": lax.rem(x + nx - 1, nx)}]
    for peer in peers:
        pl.semaphore_signal(barrier, inc=1, device_id=peer, device_id_type=MESH)

    @pl.when(root)
    def _():
        @pl.loop(1, nx * nz)
        def _(i):
            pl.semaphore_signal(barrier, inc=1, device_id={"row": i // nz, "col": lax.rem(i, nz)}, device_id_type=MESH)

    @pl.when(jnp.logical_not(root))
    def _():
        pl.semaphore_signal(barrier, inc=1, device_id={"row": 0, "col": 0}, device_id_type=MESH)

    for copy in local[:6]:
        copy.wait()
    lsrc[:, whole:rows] = rbuf[depth, :, whole:rows]

    @pl.when(root)
    def _():
        pl.semaphore_wait(barrier, len(peers) + nx * nz - 1)

    @pl.when(jnp.logical_not(root))
    def _():
        pl.semaphore_wait(barrier, len(peers) + 1)

    def mrings(who):
        if who == 0:
            small = Ring(nz, z, "col", lambda i, c: mbuf.at[0, x, i, :, cols(c)], ms_send, ms_recv)
            bulk = Ring(nx, x, "row", lambda i, c: mbuf.at[0, i, :, :, cols(c)], mb_send, mb_recv)
        else:
            small = Ring(nx, x, "row", lambda i, c: mbuf.at[1, i, z, :, cols(c)], ms_send, ms_recv)
            bulk = Ring(nz, z, "col", lambda i, c: mbuf.at[1, :, i, :, cols(c)], mb_send, mb_recv)
        return small, bulk

    def lpart(c, i, j):
        return lbuf.at[c, pl.ds(pl.multiple_of(i * lx, lx), lx), pl.ds(pl.multiple_of(j * lz, lz), lz)]

    def lrings(who):
        if who == 0:
            small = Ring(nz, z, "col", lambda i, c: lpart(c, x, i), ls_send, ls_recv)
            bulk = Ring(nx, x, "row", lambda i, c: lbuf.at[c, pl.ds(pl.multiple_of(i * lx, lx), lx)], lb_send, lb_recv)
        else:
            small = Ring(nx, x, "row", lambda i, c: lpart(c, i, z), ls_send, ls_recv)
            bulk = Ring(nz, z, "col", lambda i, c: lbuf.at[c, :, pl.ds(pl.multiple_of(i * lz, lz), lz)], lb_send, lb_recv)
        return small, bulk

    rring = Ring(ny, y, "depth_y", lambda i, c: rbuf.at[i * 2 + core, c], rsend, rrecv)

    def rcopy(way, step, chunk, incoming=False):
        sign = 1 if way == 0 else -1
        hops = step if incoming else step - 1
        origin = lax.rem(y - sign * hops + ny, ny)
        target = lax.rem(y + sign + ny, ny)
        k = rring.index(way, step, chunk)
        ref = rbuf.at[origin * 2 + core, chunk]
        return remote(ref, ref, rsend.at[k], rrecv.at[k], {"depth": target * 2 + core})

    rring.copy = rcopy

    def slot_relay(i, c, k, mine=True):
        ref = rbuf.at[i * 2 + (core if mine else 1 - core), c]
        return remote(ref, ref, dr_send.at[k], dr_recv.at[k], {"depth": other})

    def ring_origin(way, step):
        return lax.rem(y - (step if way == 0 else -step) + ny, ny)

    def rrelay(way, step, chunk, mine=True):
        return slot_relay(ring_origin(way, step), chunk, 2 + rring.index(way, step, chunk), mine)

    def mrelay(ring, way, step, chunk):
        origin = ring.me if step == 0 else lax.rem(ring.me - (step if way == 0 else -step) + ring.n, ring.n)
        ref = ring.block(origin, chunk)
        k = chunk if step == 0 else 2 + ring.index(way, step, chunk)
        return remote(ref, ref, dm_send.at[k], dm_recv.at[k], {"depth": other})

    def mkeys(ring):
        keys = [(0, 0, 0), (0, 0, 1)]
        for step in range(1, ring.steps + 1):
            keys += ring.order(step)
        return keys

    trade = remote(rows4.at[1 - core], swap, sw_send, sw_recv, {"depth": other})
    trade.start()
    for c in range(2):
        slot_relay(y, c, c).start()
    trade.wait_recv()
    own, got = rows4[core], swap[...]
    first = core == 0
    tile = jnp.concatenate([jnp.where(first, own, got), jnp.where(first, got, own)], axis=0)

    def mrow(i):
        return mbuf.at[core, x, z, pl.ds(pl.multiple_of(i * 8, 8), 8)]

    mbuf[core, x, z, pl.ds(pl.multiple_of(y * 8, 8), 8), :] = tile

    def piece(i, j):
        return (pl.ds(0, 2), pl.ds(pl.multiple_of(i * lx, lx), lx), pl.ds(pl.multiple_of(j * lz, lz), lz))

    def scatter(i, j):
        return remote(lsrc.at[piece(i, j)], lbuf.at[piece(i, j)], sc_send.at[i * nz + j], sc_recv, {"row": i, "col": j})

    def ycopy(j, incoming=False):
        ref = mrow(lax.rem(y + ny - j, ny) if incoming else y)
        return remote(ref, ref, ysend.at[j], yrecv.at[j], {"depth": lax.rem(y + j, ny) * 2 + core})

    for j in range(1, ny):
        ycopy(j).start()
    rring.start(1)

    @pl.when(root)
    def _():
        lbuf[:, 0:lx, 0:lz] = lsrc[:, 0:lx, 0:lz]

        @pl.loop(1, nx * nz)
        def _(i):
            scatter(i // nz, lax.rem(i, nz)).start()

    for j in range(1, ny):
        ycopy(j, incoming=True).wait_recv()

    def gather(who):
        small, bulk = mrings(who)
        lsmall, lbulk = lrings(who)
        small.run()
        bulk.start(1)
        for c in range(2):
            mrelay(bulk, 0, 0, c).start()

        @pl.when(jnp.logical_not(root))
        def _():
            scatter(x, z).wait_recv()

        lsmall.run()
        bulk.take(1, lambda *key: mrelay(bulk, *key).start())
        lbulk.start(1)
        for key in rring.order(1):
            rring.arrived(*key)
            rring.forward(*key)
            rrelay(*key).start()
        for step in range(2, bulk.steps + 1):
            bulk.take(step, lambda *key: mrelay(bulk, *key).start())
        for step in range(1, lbulk.steps + 1):
            lbulk.take(step)
        theirs = mrings(1 - who)[1]
        for key in mkeys(theirs):
            mrelay(theirs, *key).wait_recv()

    for who in range(2):
        @pl.when(core == who)
        def _():
            gather(who)

    block = mbuf.shape[3]

    @pl.loop(0, nx * nz)
    def _(i):
        at = pl.ds(pl.multiple_of(i * block, block), block)
        whi[at], wlo[at] = split(mbuf[0, i // nz, lax.rem(i, nz)])
        shi[at], slo[at] = split(mbuf[1, i // nz, lax.rem(i, nz)])

    tile_rows = yhi.shape[0]
    nt = half

    @pl.loop(0, width // tile_rows)
    def _(i):
        at = pl.ds(pl.multiple_of(i * tile_rows, tile_rows), tile_rows)

        @pl.loop(0, width // nt)
        def _(j):
            to = pl.ds(pl.multiple_of(j * nt, nt), nt)
            yhi[:, to], ylo[:, to] = split(dot3(whi[at], wlo[at], shi[:, to], slo[:, to], NN))

        @pl.loop(0, width // nt)
        def _(j):
            to = pl.ds(pl.multiple_of(j * nt, nt), nt)
            out = dot3(yhi[...], ylo[...], whi[to], wlo[to], NT)
            cblk[:, to] = out
            chi[at, to], clo[at, to] = split(out)

        chip = (x * nz + z) * ny + y

        @pl.when(chip // (tile_rows // 8) == i)
        def _():
            mine = cblk[pl.ds(pl.multiple_of(lax.rem(chip, tile_rows // 8) * 8, 8), 8), :]
            cbuf[...] = jnp.where(first, mine[0:4], mine[4:8])

    c_copy = pltpu.make_async_copy(cbuf, c_out, load.at[0])
    c_copy.start()

    def split_rows(i):
        for c in range(2):
            rhi[i, c, 0:rows], rlo[i, c, 0:rows] = split(rbuf[i, c])

    split_rows(depth)
    for c in range(2):
        lhi[c], llo[c] = split(lbuf[c])

    @pl.loop(0, width // nt)
    def _(j):
        to = pl.ds(pl.multiple_of(j * nt, nt), nt)
        out = dot3(rhi[depth, 0], rlo[depth, 0], whi[to], wlo[to], NT)
        out = out - dot3(rhi[depth, 1], rlo[depth, 1], chi[:, to], clo[:, to], NN)
        pbuf[:, to] = out[0:rows]
        out = dot3(lhi[0], llo[0], whi[to], wlo[to], NT)
        out = out - dot3(lhi[1], llo[1], chi[:, to], clo[:, to], NN)
        pq_hi[1, :, to], pq_lo[1, :, to] = split(out)
        out = dot3(lhi[1], llo[1], whi[:, to], wlo[:, to], NN)
        pq_hi[0, :, to], pq_lo[0, :, to] = split(out)

    p_copy = pltpu.make_async_copy(pbuf, p_out, load.at[1])
    p_copy.start()

    for step in range(2, rring.steps + 1):
        for key in rring.order(step):
            rring.arrived(*key)
            rrelay(*key).start()
    for c in range(2):
        slot_relay(y, c, c, mine=False).wait_recv()
    for step in range(1, rring.steps + 1):
        for key in rring.order(step):
            rrelay(*key, mine=False).wait_recv()

    @pl.loop(0, nd)
    def _(i):
        @pl.when(i != depth)
        def _():
            split_rows(i)

        out = dot3(pq_hi[0], pq_lo[0], rhi[i, 0], rlo[i, 0], NT)
        ubuf[i, :, 0:rhi.shape[2]] = out + dot3(pq_hi[1], pq_lo[1], rhi[i, 1], rlo[i, 1], NT)

    local[6].wait()

    def rest(at):
        update = jnp.concatenate([ubuf[i, at, 0:rows] for i in range(nd)], axis=1)
        tbuf[at, :] = tbuf[at, :] - update

    @pl.loop(0, rows // 8)
    def _(i):
        rest(pl.ds(pl.multiple_of(i * 8, 8), 8))

    rest(slice(whole, rows))
    t_copy = pltpu.make_async_copy(tbuf, t_out, load.at[2])
    t_copy.start()

    trade.wait_send()
    for c in range(2):
        slot_relay(y, c, c).wait_send()
    for j in range(1, ny):
        ycopy(j).wait_send()
    rring.drain()
    for step in range(1, rring.steps + 1):
        for key in rring.order(step):
            rrelay(*key).wait_send()

    @pl.when(root)
    def _():
        @pl.loop(1, nx * nz)
        def _(i):
            scatter(i // nz, lax.rem(i, nz)).wait_send()

    for who in range(2):
        @pl.when(core == who)
        def _():
            small, bulk = mrings(who)
            lsmall, lbulk = lrings(who)
            for ring in (small, bulk, lsmall, lbulk):
                ring.drain()
            for key in mkeys(bulk):
                mrelay(bulk, *key).wait_send()

    c_copy.wait()
    p_copy.wait()
    t_copy.wait()


def body(dims, trailing, panel_block, factor_panel, corner_block, corner_inverse):
    nx, nz, ny = dims
    nd = 2 * ny
    rows, width = panel_block.shape
    pad = -(-rows // (8 * nx)) * 8 * nx
    padded = -(-rows // 16) * 16
    pad = max(pad, padded)
    corner_rows = corner_block.shape[0]
    big = max(nx, nz)
    sems = pltpu.SemaphoreType.DMA
    vmem = pltpu.VMEM
    any_space = pl.BlockSpec(memory_space=pl.ANY)
    tile_rows = min(256, width // 2)
    scratch = [
        vmem((nd, 2, rows, width), F32),
        vmem((nd, 2, padded, width), BF16), vmem((nd, 2, padded, width), BF16),
        vmem((2, pad, width), F32), vmem((2, pad, width), F32),
        vmem((2, pad, width), BF16), vmem((2, pad, width), BF16),
        vmem((2, nx, nz, 8 * ny, width), F32),
        vmem((2, corner_rows, width), F32), vmem((corner_rows, width), F32),
        vmem((width, width), BF16), vmem((width, width), BF16),
        vmem((width, width), BF16), vmem((width, width), BF16),
        vmem((width, width), BF16), vmem((width, width), BF16),
        vmem((tile_rows, width), BF16), vmem((tile_rows, width), BF16),
        vmem((tile_rows, width), F32),
        vmem((2, pad, width), BF16), vmem((2, pad, width), BF16),
        vmem((rows, width), F32),
        vmem((nd, pad, 256), F32),
        vmem(trailing.shape, F32),
        vmem((corner_rows, width), F32),
        sems((7,)), sems((ny,)), sems((ny,)), sems((2 * ny,)), sems((2 * ny,)),
        *[sems((2 * big,)) for _ in range(8)],
        sems((2 * ny + 2,)), sems((2 * ny + 2,)), sems((2 * big + 2,)), sems((2 * big + 2,)),
        sems(()), sems(()), sems((nx * nz,)), sems(()),
    ]
    return pl.pallas_call(
        functools.partial(kernel, dims),
        out_shape=(
            jax.ShapeDtypeStruct(trailing.shape, F32),
            jax.ShapeDtypeStruct(panel_block.shape, F32),
            jax.ShapeDtypeStruct(corner_block.shape, F32),
        ),
        in_specs=[any_space] * 5,
        out_specs=(any_space,) * 3,
        scratch_shapes=scratch,
        compiler_params=pltpu.CompilerParams(
            collective_id=0, has_side_effects=True, vmem_limit_bytes=67_000_000
        ),
        name="panel_step",
    )(trailing, panel_block, factor_panel, corner_block, corner_inverse)


def solution(mesh):
    dims = (mesh.shape["row"], mesh.shape["col"], mesh.shape["depth"] // 2)
    columns = P("depth", ("row", "col"))
    spread = P(("row", "col", "depth"), None)
    return jax.shard_map(
        functools.partial(body, dims),
        mesh=mesh,
        in_specs=(columns, spread, spread, spread, spread),
        out_specs=(columns, spread, spread),
        check_vma=False,
    )
```

```python
import functools

import jax
import jax.numpy as jnp
from jax import lax
from jax.experimental import pallas as pl
from jax.experimental.pallas import tpu as pltpu
from jax.sharding import PartitionSpec as P

F32, BF16 = jnp.float32, jnp.bfloat16
MESH = pl.DeviceIdType.MESH
NN = (((1,), (0,)), ((), ()))
NT = (((1,), (1,)), ((), ()))


def split(x):
    hi = x.astype(BF16)
    return hi, (x - hi.astype(F32)).astype(BF16)


def dot3(a, b, dims):
    (ah, al), (bh, bl) = a, b
    dot = functools.partial(lax.dot_general, dimension_numbers=dims, preferred_element_type=F32)
    return dot(ah, bh) + dot(ah, bl) + dot(al, bh)


def remote(src, dst, send, recv, device):
    return pltpu.make_async_remote_copy(
        src_ref=src, dst_ref=dst, send_sem=send, recv_sem=recv, device_id=device, device_id_type=MESH
    )


class Direct:
    def __init__(self, n, me, device, block, send, recv):
        self.n, self.me, self.device, self.block, self.send, self.recv = n, me, device, block, send, recv

    def copy(self, j, incoming=False):
        ref = self.block(lax.rem(self.me + self.n - j, self.n) if incoming else self.me)
        return remote(ref, ref, self.send.at[j], self.recv.at[j], self.device(lax.rem(self.me + j, self.n)))

    def start(self):
        for j in sorted(range(1, self.n), key=lambda j: -min(j, self.n - j)):
            self.copy(j).start()

    def take(self):
        for j in range(1, self.n):
            self.copy(j, incoming=True).wait_recv()

    def drain(self):
        for j in range(1, self.n):
            self.copy(j).wait_send()


class Ring:
    def __init__(self, n, me, device, block, counts, send, recv):
        self.n, self.me, self.device, self.block, self.counts = n, me, device, block, counts
        self.send, self.recv, self.steps = send, recv, n // 2

    def keys(self, step):
        out = []
        for at in range(2):
            for way in range(2):
                chunk = at if way == 0 else 1 - at
                if step < self.steps or chunk == way:
                    out += [(way, step, chunk, piece) for piece in range(self.counts[chunk])]
        return out

    def index(self, way, step, chunk, piece):
        return ((way * self.steps + step - 1) * 2 + chunk) * 2 + piece

    def origin(self, way, hops):
        return lax.rem(self.me - (hops if way == 0 else -hops) + self.n, self.n)

    def copy(self, way, step, chunk, piece, incoming=False):
        ref = self.block(self.origin(way, step if incoming else step - 1), chunk, piece)
        target = lax.rem(self.me + (1 if way == 0 else -1) + self.n, self.n)
        k = self.index(way, step, chunk, piece)
        return remote(ref, ref, self.send.at[k], self.recv.at[k], self.device(target))

    def start(self):
        for key in self.keys(1):
            self.copy(*key).start()

    def take(self, step, then=None, keys=None):
        for key in self.keys(step) if keys is None else keys:
            way, step, chunk, piece = key
            self.copy(*key, incoming=True).wait_recv()
            if step < self.steps and (step + 1 < self.steps or chunk == way):
                self.copy(way, step + 1, chunk, piece).start()
            if then is not None:
                then(*key)

    def drain(self):
        for step in range(1, self.steps + 1):
            for key in self.keys(step):
                self.copy(*key).wait_send()


class Relay:
    def __init__(self, ring, theirs, device, send, recv):
        self.ring, self.theirs, self.device, self.send, self.recv = ring, theirs, device, send, recv

    def own(self):
        counts = self.ring.counts
        return [(0, 0, chunk, piece) for chunk in range(2) for piece in range(counts[chunk])]

    def copy(self, way, step, chunk, piece, incoming=False):
        ref = (self.theirs if incoming else self.ring.block)(self.ring.origin(way, step), chunk, piece)
        k = chunk * 2 + piece if step == 0 else 4 + self.ring.index(way, step, chunk, piece)
        return remote(ref, ref, self.send.at[k], self.recv.at[k], self.device)

    def start(self, *key):
        self.copy(*key).start()

    def start_own(self):
        for key in self.own():
            self.copy(*key).start()

    def take(self, *keys):
        for key in keys:
            self.copy(*key, incoming=True).wait_recv()

    def every(self):
        return self.own() + [key for step in range(1, self.ring.steps + 1) for key in self.ring.keys(step)]

    def drain(self):
        for key in self.every():
            self.copy(*key).wait_send()


def kernel(
    dims, trailing, a_in, f_in, s_in, w_in, t_out, p_out, c_out,
    rbuf, rhi, rlo, lsrc, lbuf, phi, plo, mbuf, rows4, swap, whi, wlo, shi, slo, yhi, ylo, chi, clo,
    qhi, qlo, pbuf, ubuf, tbuf, cbuf,
    load, ysend, yrecv, rsend, rrecv, xs_send, xs_recv, zs_send, zs_recv, zb_send, zb_recv, xb_send, xb_recv,
    ls_send, ls_recv, lb_send, lb_recv, dr_send, dr_recv, dz_send, dz_recv, dx_send, dx_recv,
    sw_send, sw_recv, lx_send, lx_recv, lz_send, lz_recv,
):
    nx, nz, ny = dims
    nd = 2 * ny
    rows, width = a_in.shape
    whole = rows // 8 * 8
    x, z, depth = lax.axis_index("row"), lax.axis_index("col"), lax.axis_index("depth")
    y, core = depth // 2, lax.rem(depth, 2)
    pad = lbuf.shape[1]
    lx, lz = pad // nx, width // nz
    unit, half = width // nx, width // 2
    on_edge, on_side = z == 0, x == 0
    root = jnp.logical_and(on_edge, on_side)
    partner = {"depth": y * 2 + 1 - core}

    def on_x(i):
        return {"row": i}

    def on_y(i):
        return {"depth": i * 2 + core}

    def on_z(i):
        return {"col": i}

    def tile(i, size):
        return pl.ds(pl.multiple_of(i * size, size), size)

    def line(c, i):
        return lsrc.at[c, tile(i, lx)], lbuf.at[c, tile(i, lx)]

    def lscatter(c, i):
        src, dst = line(c, i)
        return remote(src, dst, lx_send.at[c * nx + i], lx_recv.at[c], on_x(i))

    def part(c, j):
        return lbuf.at[c, tile(x, lx), tile(j, lz)]

    def zscatter(c, j):
        return remote(part(c, j), part(c, j), lz_send.at[c * nz + j], lz_recv.at[c], on_z(j))

    def lsmall(c, j, incoming=False):
        ref = part(c, lax.rem(z + nz - j, nz) if incoming else z)
        return remote(ref, ref, ls_send.at[c * nz + j], ls_recv.at[c * nz + j], on_z(lax.rem(z + j, nz)))

    def lsmall_sends(c, act):
        for j in range(1, nz):
            @pl.when(lax.rem(z + j, nz) != 0)
            def _():
                act(lsmall(c, j))

    def edge(c):
        @pl.when(on_edge)
        def _():
            @pl.when(jnp.logical_not(on_side))
            def _():
                lscatter(c, x).wait_recv()

            for j in range(1, nz):
                zscatter(c, j).start()
            lsmall_sends(c, lambda copy: copy.start())

    def inner(c):
        @pl.when(jnp.logical_not(on_edge))
        def _():
            zscatter(c, z).wait_recv()
            lsmall_sends(c, lambda copy: copy.start())

    def gathered(c):
        @pl.when(jnp.logical_not(on_edge))
        def _():
            for j in range(1, nz):
                lsmall(c, j, incoming=True).wait_recv()

        for key in lbulk.keys(1):
            if key[2] == c:
                lbulk.copy(*key).start()

    lbulk = Ring(nx, x, on_x, lambda i, chunk, piece: lbuf.at[chunk, tile(i, lx)], (1, 1), lb_send, lb_recv)

    loads = [
        (w_in, rows4.at[0]),
        (s_in, rows4.at[1]),
        (a_in, rbuf.at[depth, 0]),
        (f_in, rbuf.at[depth, 1]),
        (a_in.at[pl.ds(0, whole)], lsrc.at[0, pl.ds(0, whole)]),
        (f_in.at[pl.ds(0, whole)], lsrc.at[1, pl.ds(0, whole)]),
        (trailing, tbuf),
    ]
    local = [pltpu.make_async_copy(src, dst, load.at[i]) for i, (src, dst) in enumerate(loads)]
    for copy in local:
        copy.start()

    barrier = pltpu.get_barrier_semaphore()
    peers = [partner]
    peers += [on_y(lax.rem(y + j, ny)) for j in range(1, ny)]
    peers += [on_x(lax.rem(x + j, nx)) for j in range(1, nx)]
    peers += [on_z(lax.rem(z + j, nz)) for j in range(1, nz)]
    for peer in peers:
        pl.semaphore_signal(barrier, inc=1, device_id=peer, device_id_type=MESH)

    for copy in local[:6]:
        copy.wait()
    lsrc[:, whole:rows] = rbuf[depth, :, whole:rows]

    pl.semaphore_wait(barrier, len(peers))

    trade = remote(rows4.at[1 - core], swap, sw_send, sw_recv, partner)
    trade.start()

    def panel(who):
        return lambda i, chunk, piece: rbuf.at[i * 2 + who, chunk, :, pl.ds(piece * half, half)]

    rring = Ring(ny, y, on_y, panel(core), (2, 2), rsend, rrecv)
    rrelay = Relay(rring, panel(1 - core), partner, dr_send, dr_recv)

    def myrow(i):
        return mbuf.at[core, x, z, tile(i, 8)]

    ysmall = Direct(ny, y, on_y, myrow, ysend, yrecv)

    @pl.when(root)
    def _():
        for c in range(2):
            for i in range(1, nx):
                lscatter(c, i).start()
        lbuf[:, 0:lx] = lsrc[:, 0:lx]

    trade.wait_recv()
    own, got = rows4[core], swap[...]
    first = core == 0
    mbuf[core, x, z, tile(y, 8), :] = jnp.concatenate(
        [jnp.where(first, own, got), jnp.where(first, got, own)], axis=0
    )
    ysmall.start()
    rring.start()

    def split_slot(i):
        for c in range(2):
            rhi[i, c, 0:rows], rlo[i, c, 0:rows] = split(rbuf[i, c])

    split_slot(depth)
    for c in range(2):
        phi[c, 0:rows] = rhi[depth, c, 0:rows]
        plo[c, 0:rows] = rlo[depth, c, 0:rows]

    rest = pl.ds(unit, width - unit)
    xsmall = Direct(nx, x, on_x, lambda i: mbuf.at[core, i, z, :, rest], xs_send, xs_recv)
    zsmall = Direct(nz, z, on_z, lambda i: mbuf.at[core, x, i, :, pl.ds(0, unit)], zs_send, zs_recv)
    layout = ([nx - 1], list(range(nx - 2, 0, -1)))

    def zblock(who):
        def block(i, chunk, piece):
            at = layout[chunk][piece]
            return mbuf.at[who, at, i, :, pl.ds(unit, at * unit)]
        return block

    def xblock(who):
        return lambda i, chunk, piece: mbuf.at[who, i, pl.ds(chunk * (nz // 2), nz // 2), :, pl.ds(0, unit)]

    zbulk = Ring(nz, z, on_z, zblock(core), tuple(len(part) for part in layout), zb_send, zb_recv)
    zrelay = Relay(zbulk, zblock(1 - core), partner, dz_send, dz_recv)
    xbulk = Ring(nx, x, on_x, xblock(core), (1, 1), xb_send, xb_recv)
    xrelay = Relay(xbulk, xblock(1 - core), partner, dx_send, dx_recv)

    ysmall.take()
    xsmall.start()
    zsmall.start()
    rrelay.start_own()
    edge(0)
    xsmall.take()
    zbulk.start()
    zrelay.start_own()
    zsmall.take()
    xbulk.start()
    xrelay.start_own()
    inner(0)
    edge(1)
    zbulk.take(1, zrelay.start)
    xbulk.take(1, xrelay.start)
    inner(1)
    if zbulk.steps > 1:
        zbulk.take(2, zrelay.start)
    early = [key for key in rring.keys(1) if key[2] == key[0]]
    late = [key for key in rring.keys(1) if key[2] != key[0]]
    rring.take(1, rrelay.start, early)
    gathered(0)
    if zbulk.steps > 2:
        zbulk.take(3, zrelay.start)
    for step in range(2, xbulk.steps + 1):
        xbulk.take(step, xrelay.start)
    gathered(1)
    for step in range(4, zbulk.steps + 1):
        zbulk.take(step, zrelay.start)
    zrelay.take(*zrelay.every())
    xrelay.take(*xrelay.every())
    lbulk.take(1)
    block = mbuf.shape[3]

    @pl.loop(0, nx * nz)
    def _(i):
        at = tile(i, block)
        whi[at], wlo[at] = split(mbuf[0, i // nz, lax.rem(i, nz)])
        shi[at], slo[at] = split(mbuf[1, i // nz, lax.rem(i, nz)])

    def cut(i, j=None):
        return slice(i * unit, (i + 1 if j is None else j) * unit)

    def pair(hi, lo, *at):
        return hi[at], lo[at]

    for i in range(nx):
        for j in range(nx):
            out = 0.0
            top = min(j, i + 1)
            if top > 0:
                out = dot3(pair(whi, wlo, cut(i), cut(0, top)), pair(shi, slo, cut(j), cut(0, top)), NT)
            if j <= i:
                out = out + dot3(pair(whi, wlo, cut(i), cut(j, i + 1)), pair(shi, slo, cut(j, i + 1), cut(j)), NN)
            yhi[cut(i), cut(j)], ylo[cut(i), cut(j)] = split(out)
    for i in range(nx):
        for j in range(i + 1):
            out = dot3(pair(yhi, ylo, cut(i), cut(0, j + 1)), pair(whi, wlo, cut(j), cut(0, j + 1)), NT)
            chi[cut(i), cut(j)], clo[cut(i), cut(j)] = split(out)
    rring.take(1, rrelay.start, late)
    rrelay.take(*rrelay.own())
    rrelay.take(*rring.keys(1))
    far = 2 if ny > 2 else 0

    def near(i):
        return lax.rem(2 * y + nd - 2 + i, nd) if far else i

    @pl.loop(0, nd - far)
    def _(i):
        @pl.when(near(i) != depth)
        def _():
            split_slot(near(i))

    for step in range(2, lbulk.steps + 1):
        lbulk.take(step)
    for c in range(2):
        phi[c, pad:2 * pad], plo[c, pad:2 * pad] = split(lbuf[c])
    both = slice(0, 2 * pad)
    slab = slice(pad, 2 * pad)
    for j in range(nx):
        out = dot3(pair(phi, plo, 0, both, cut(0, j + 1)), pair(whi, wlo, cut(j), cut(0, j + 1)), NT)
        if j > 0:
            out = out - dot3(pair(phi, plo, 1, both, cut(0, j)), pair(chi, clo, cut(j), cut(0, j)), NT)
        out = out - dot3(pair(phi, plo, 1, both, cut(j, nx)), pair(chi, clo, cut(j, nx), cut(j)), NN)
        pbuf[:, cut(j)] = out[0:rows]
        qhi[1, :, cut(j)], qlo[1, :, cut(j)] = split(out[pad:2 * pad])
        out = dot3(pair(phi, plo, 1, slab, cut(j, nx)), pair(whi, wlo, cut(j, nx), cut(j)), NN)
        qhi[0, :, cut(j)], qlo[0, :, cut(j)] = split(out)

    p_copy = pltpu.make_async_copy(pbuf, p_out, load.at[1])
    p_copy.start()

    chip = (x * nz + z) * ny + y
    at = tile(chip // 2, 16)
    mine = jnp.concatenate(
        [
            dot3(pair(yhi, ylo, at, cut(0, j + 1)), pair(whi, wlo, cut(j), cut(0, j + 1)), NT)
            for j in range(nx)
        ],
        axis=1,
    )
    mine = jnp.where(lax.rem(chip, 2) == 0, mine[0:8], mine[8:16])
    cbuf[...] = jnp.where(first, mine[0:4], mine[4:8])
    c_copy = pltpu.make_async_copy(cbuf, c_out, load.at[0])
    c_copy.start()

    def slot(i):
        out = dot3(pair(qhi, qlo, 0), pair(rhi, rlo, i, 0), NT)
        ubuf[i, :, 0:rhi.shape[2]] = out + dot3(pair(qhi, qlo, 1), pair(rhi, rlo, i, 1), NT)

    @pl.loop(0, nd - far)
    def _(i):
        slot(near(i))

    for step in range(2, rring.steps + 1):
        rring.take(step, rrelay.start)
    for step in range(2, rring.steps + 1):
        rrelay.take(*rring.keys(step))
    if far:
        @pl.loop(0, far)
        def _(i):
            at = lax.rem(2 * y + nd // 2 + i, nd)
            split_slot(at)
            slot(at)

    local[6].wait()

    def finish(at):
        update = jnp.concatenate([ubuf[i, at, 0:rows] for i in range(nd)], axis=1)
        tbuf[at, :] = tbuf[at, :] - update

    step = 32
    if rows >= step:
        @pl.loop(0, rows // step)
        def _(i):
            finish(tile(i, step))

    finish(slice(rows // step * step, rows))
    t_copy = pltpu.make_async_copy(tbuf, t_out, load.at[2])
    t_copy.start()

    trade.wait_send()
    for each in (ysmall, xsmall, zsmall, rring, zbulk, xbulk, lbulk, rrelay, zrelay, xrelay):
        each.drain()
    for c in range(2):
        lsmall_sends(c, lambda copy: copy.wait_send())

    @pl.when(on_edge)
    def _():
        for c in range(2):
            for j in range(1, nz):
                zscatter(c, j).wait_send()

    @pl.when(root)
    def _():
        for c in range(2):
            for i in range(1, nx):
                lscatter(c, i).wait_send()

    c_copy.wait()
    p_copy.wait()
    t_copy.wait()


def body(dims, trailing, panel_block, factor_panel, corner_block, corner_inverse):
    nx, nz, ny = dims
    nd = 2 * ny
    rows, width = panel_block.shape
    pad = max(-(-rows // (8 * nx)) * 8 * nx, -(-rows // 16) * 16)
    corner_rows = corner_block.shape[0]
    vmem = pltpu.VMEM
    square = vmem((width, width), BF16)
    any_space = pl.BlockSpec(memory_space=pl.ANY)

    def sems(*counts):
        return [pltpu.SemaphoreType.DMA((n,)) for n in counts for _ in range(2)]

    scratch = [
        vmem((nd, 2, rows, width), F32),
        vmem((nd, 2, pad, width), BF16), vmem((nd, 2, pad, width), BF16),
        vmem((2, pad, width), F32), vmem((2, pad, width), F32),
        vmem((2, 2 * pad, width), BF16), vmem((2, 2 * pad, width), BF16),
        vmem((2, nx, nz, 8 * ny, width), F32),
        vmem((2, corner_rows, width), F32), vmem((corner_rows, width), F32),
        *[square] * 8,
        vmem((2, pad, width), BF16), vmem((2, pad, width), BF16),
        vmem((rows, width), F32),
        vmem((nd, pad, 256), F32),
        vmem(trailing.shape, F32),
        vmem((corner_rows, width), F32),
        pltpu.SemaphoreType.DMA((7,)),
        *sems(ny, 4 * ny, nx, nz, 4 * nz, 4 * nx, 2 * nz, 4 * nx, 4 * ny + 4, 4 * nz + 4, 4 * nx + 4),
        pltpu.SemaphoreType.DMA, pltpu.SemaphoreType.DMA,
        *sems(2 * nx, 2 * nz),
    ]
    return pl.pallas_call(
        functools.partial(kernel, dims),
        out_shape=(
            jax.ShapeDtypeStruct(trailing.shape, F32),
            jax.ShapeDtypeStruct(panel_block.shape, F32),
            jax.ShapeDtypeStruct(corner_block.shape, F32),
        ),
        in_specs=[any_space] * 5,
        out_specs=(any_space,) * 3,
        scratch_shapes=scratch,
        compiler_params=pltpu.CompilerParams(
            collective_id=0, has_side_effects=True, vmem_limit_bytes=67_000_000
        ),
        name="panel_step",
    )(trailing, panel_block, factor_panel, corner_block, corner_inverse)


def solution(mesh):
    dims = (mesh.shape["row"], mesh.shape["col"], mesh.shape["depth"] // 2)
    columns = P("depth", ("row", "col"))
    spread = P(("row", "col", "depth"), None)
    return jax.shard_map(
        functools.partial(body, dims),
        mesh=mesh,
        in_specs=(columns, spread, spread, spread, spread),
        out_specs=(columns, spread, spread),
        check_vma=False,
    )
```

```python
import functools

import jax
import jax.numpy as jnp
from jax import lax
from jax.experimental import pallas as pl
from jax.experimental.pallas import tpu as pltpu
from jax.sharding import PartitionSpec as P

F32, BF16 = jnp.float32, jnp.bfloat16
MESH = pl.DeviceIdType.MESH
NN = (((1,), (0,)), ((), ()))
NT = (((1,), (1,)), ((), ()))


def split(x):
    hi = x.astype(BF16)
    return hi, (x - hi.astype(F32)).astype(BF16)


def dot3(a, b, dims):
    (ah, al), (bh, bl) = a, b
    dot = functools.partial(lax.dot_general, dimension_numbers=dims, preferred_element_type=F32)
    return dot(ah, bh) + dot(ah, bl) + dot(al, bh)


def remote(src, dst, send, recv, device):
    return pltpu.make_async_remote_copy(
        src_ref=src, dst_ref=dst, send_sem=send, recv_sem=recv, device_id=device, device_id_type=MESH
    )


class Direct:
    def __init__(self, n, me, device, block, send, recv):
        self.n, self.me, self.device, self.block, self.send, self.recv = n, me, device, block, send, recv

    def copy(self, j, incoming=False):
        ref = self.block(lax.rem(self.me + self.n - j, self.n) if incoming else self.me)
        return remote(ref, ref, self.send.at[j], self.recv.at[j], self.device(lax.rem(self.me + j, self.n)))

    def start(self):
        for j in sorted(range(1, self.n), key=lambda j: -min(j, self.n - j)):
            self.copy(j).start()

    def take(self):
        for j in range(1, self.n):
            self.copy(j, incoming=True).wait_recv()

    def drain(self):
        for j in range(1, self.n):
            self.copy(j).wait_send()


class Ring:
    def __init__(self, n, me, device, block, counts, send, recv):
        self.n, self.me, self.device, self.block, self.counts = n, me, device, block, counts
        self.send, self.recv, self.steps = send, recv, n // 2

    def keys(self, step):
        out = []
        for at in range(2):
            for way in range(2):
                chunk = at if way == 0 else 1 - at
                if step < self.steps or chunk == way:
                    out += [(way, step, chunk, piece) for piece in range(self.counts[chunk])]
        return out

    def index(self, way, step, chunk, piece):
        return ((way * self.steps + step - 1) * 2 + chunk) * 2 + piece

    def origin(self, way, hops):
        return lax.rem(self.me - (hops if way == 0 else -hops) + self.n, self.n)

    def copy(self, way, step, chunk, piece, incoming=False):
        ref = self.block(self.origin(way, step if incoming else step - 1), chunk, piece)
        target = lax.rem(self.me + (1 if way == 0 else -1) + self.n, self.n)
        k = self.index(way, step, chunk, piece)
        return remote(ref, ref, self.send.at[k], self.recv.at[k], self.device(target))

    def start(self, chunk=None):
        for key in self.keys(1):
            if chunk in (None, key[2]):
                self.copy(*key).start()

    def take(self, step, then=None, keys=None, only=None):
        if step > self.steps:
            return
        for key in self.keys(step) if keys is None else keys:
            if only not in (None, key[2]):
                continue
            way, step, chunk, piece = key
            self.copy(*key, incoming=True).wait_recv()
            if step < self.steps and (step + 1 < self.steps or chunk == way):
                self.copy(way, step + 1, chunk, piece).start()
            if then is not None:
                then(*key)

    def drain(self):
        for step in range(1, self.steps + 1):
            for key in self.keys(step):
                self.copy(*key).wait_send()


class Relay:
    def __init__(self, ring, theirs, device, send, recv):
        self.ring, self.theirs, self.device, self.send, self.recv = ring, theirs, device, send, recv

    def own(self):
        counts = self.ring.counts
        return [(0, 0, chunk, piece) for chunk in range(2) for piece in range(counts[chunk])]

    def copy(self, way, step, chunk, piece, incoming=False):
        ref = (self.theirs if incoming else self.ring.block)(self.ring.origin(way, step), chunk, piece)
        k = chunk * 2 + piece if step == 0 else 4 + self.ring.index(way, step, chunk, piece)
        return remote(ref, ref, self.send.at[k], self.recv.at[k], self.device)

    def start(self, *key):
        self.copy(*key).start()

    def start_own(self):
        for key in self.own():
            self.copy(*key).start()

    def take(self, *keys):
        for key in keys:
            self.copy(*key, incoming=True).wait_recv()

    def every(self):
        return self.own() + [key for step in range(1, self.ring.steps + 1) for key in self.ring.keys(step)]

    def drain(self):
        for key in self.every():
            self.copy(*key).wait_send()


def kernel(
    dims, trailing, a_in, f_in, s_in, w_in, t_out, p_out, c_out,
    rbuf, rhi, rlo, lsrc, lline, lbuf, phi, plo, mbuf, rows4, swap, whi, wlo, shi, slo, yhi, ylo, chi, clo,
    qhi, qlo, pbuf, ubuf, tbuf, cbuf,
    load, ysend, yrecv, rsend, rrecv, xs_send, xs_recv, zs_send, zs_recv, zb_send, zb_recv, xb_send, xb_recv,
    ls_send, ls_recv, lb_send, lb_recv, dr_send, dr_recv, dz_send, dz_recv, dx_send, dx_recv,
    sw_send, sw_recv, lx_send, lx_recv, lz_send, lz_recv,
):
    nx, nz, ny = dims
    nd = 2 * ny
    rows, width = a_in.shape
    whole = rows // 8 * 8
    x, z, depth = lax.axis_index("row"), lax.axis_index("col"), lax.axis_index("depth")
    y, core = depth // 2, lax.rem(depth, 2)
    pad = lbuf.shape[1]
    lx, lz = pad // nx, width // nz
    unit, half = width // nx, width // 2
    on_edge, on_side = z == 0, x == 0
    root = jnp.logical_and(on_edge, on_side)
    partner = {"depth": y * 2 + 1 - core}

    def on_x(i):
        return {"row": i}

    def on_y(i):
        return {"depth": i * 2 + core}

    def on_z(i):
        return {"col": i}

    def tile(i, size):
        return pl.ds(pl.multiple_of(i * size, size), size)

    def lscatter(c, i):
        return remote(lsrc.at[c, tile(i, lx)], lline.at[c], lx_send.at[c * nx + i], lx_recv.at[c], on_x(i))

    def zscatter(c, j):
        at = tile(j, lz)
        return remote(lline.at[c, :, at], lbuf.at[c, tile(x, lx), at], lz_send.at[c * nz + j], lz_recv.at[c], on_z(j))

    def edge(c):
        @pl.when(on_edge)
        def _():
            @pl.when(jnp.logical_not(on_side))
            def _():
                lscatter(c, x).wait_recv()

            for j in range(1, nz):
                zscatter(c, j).start()
            lbuf[c, tile(x, lx), 0:lz] = lline[c, :, 0:lz]

    def inner(c):
        @pl.when(jnp.logical_not(on_edge))
        def _():
            zscatter(c, z).wait_recv()

        lsmall.start(c)

    lsmall = Ring(nz, z, on_z, lambda i, chunk, piece: lbuf.at[chunk, tile(x, lx), tile(i, lz)], (1, 1), ls_send, ls_recv)
    lbulk = Ring(nx, x, on_x, lambda i, chunk, piece: lbuf.at[chunk, tile(i, lx)], (1, 1), lb_send, lb_recv)

    loads = [
        (w_in, rows4.at[0]),
        (s_in, rows4.at[1]),
        (a_in, rbuf.at[depth, 0]),
        (f_in, rbuf.at[depth, 1]),
        (a_in.at[pl.ds(0, whole)], lsrc.at[0, pl.ds(0, whole)]),
        (f_in.at[pl.ds(0, whole)], lsrc.at[1, pl.ds(0, whole)]),
        (trailing, tbuf),
    ]
    local = [pltpu.make_async_copy(src, dst, load.at[i]) for i, (src, dst) in enumerate(loads)]
    for copy in local:
        copy.start()

    barrier = pltpu.get_barrier_semaphore()
    peers = [partner]
    peers += [on_y(lax.rem(y + j, ny)) for j in range(1, ny)]
    peers += [on_x(lax.rem(x + j, nx)) for j in range(1, nx)]
    peers += [on_z(lax.rem(z + j, nz)) for j in range(1, nz)]
    for peer in peers:
        pl.semaphore_signal(barrier, inc=1, device_id=peer, device_id_type=MESH)

    for copy in local[:6]:
        copy.wait()
    lsrc[:, whole:rows] = rbuf[depth, :, whole:rows]

    pl.semaphore_wait(barrier, len(peers))

    trade = remote(rows4.at[1 - core], swap, sw_send, sw_recv, partner)
    trade.start()

    def panel(who):
        return lambda i, chunk, piece: rbuf.at[i * 2 + who, chunk, :, pl.ds(piece * half, half)]

    rring = Ring(ny, y, on_y, panel(core), (2, 2), rsend, rrecv)
    rrelay = Relay(rring, panel(1 - core), partner, dr_send, dr_recv)

    def myrow(i):
        return mbuf.at[core, x, z, tile(i, 8)]

    ysmall = Direct(ny, y, on_y, myrow, ysend, yrecv)

    @pl.when(root)
    def _():
        for c in range(2):
            for i in range(1, nx):
                lscatter(c, i).start()
        lline[...] = lsrc[:, 0:lx]

    trade.wait_recv()
    own, got = rows4[core], swap[...]
    first = core == 0
    mbuf[core, x, z, tile(y, 8), :] = jnp.concatenate(
        [jnp.where(first, own, got), jnp.where(first, got, own)], axis=0
    )
    ysmall.start()
    rring.start()

    def split_slot(i):
        for c in range(2):
            rhi[i, c, 0:rows], rlo[i, c, 0:rows] = split(rbuf[i, c])

    split_slot(depth)
    for c in range(2):
        phi[c, 0:rows] = rhi[depth, c, 0:rows]
        plo[c, 0:rows] = rlo[depth, c, 0:rows]

    rest = pl.ds(unit, width - unit)
    xsmall = Direct(nx, x, on_x, lambda i: mbuf.at[core, i, z, :, rest], xs_send, xs_recv)
    zsmall = Ring(
        nz, z, on_z, lambda i, chunk, piece: mbuf.at[core, x, i, :, pl.ds(chunk * (unit // 2), unit // 2)], (1, 1),
        zs_send, zs_recv,
    )
    layout = ([nx - 1], list(range(nx - 2, 0, -1)))

    def zblock(who):
        def block(i, chunk, piece):
            at = layout[chunk][piece]
            return mbuf.at[who, at, i, :, pl.ds(unit, at * unit)]
        return block

    def xblock(who):
        return lambda i, chunk, piece: mbuf.at[who, i, pl.ds(chunk * (nz // 2), nz // 2), :, pl.ds(0, unit)]

    zbulk = Ring(nz, z, on_z, zblock(core), tuple(len(part) for part in layout), zb_send, zb_recv)
    zrelay = Relay(zbulk, zblock(1 - core), partner, dz_send, dz_recv)
    xbulk = Ring(nx, x, on_x, xblock(core), (1, 1), xb_send, xb_recv)
    xrelay = Relay(xbulk, xblock(1 - core), partner, dx_send, dx_recv)

    ysmall.take()
    xsmall.start()
    zsmall.start()
    rrelay.start_own()
    zsmall.take(1)
    edge(0)
    zsmall.take(2)
    xsmall.take()
    zbulk.start()
    zrelay.start_own()
    for step in range(3, zsmall.steps + 1):
        zsmall.take(step)
    xbulk.start()
    xrelay.start_own()
    inner(0)
    edge(1)
    zbulk.take(1, zrelay.start)
    lsmall.take(1, only=0)
    inner(1)
    zbulk.take(2, zrelay.start)
    lsmall.take(2, only=0)
    lsmall.take(1, only=1)
    xbulk.take(1, xrelay.start)
    early = [key for key in rring.keys(1) if key[2] == key[0]]
    late = [key for key in rring.keys(1) if key[2] != key[0]]
    rring.take(1, rrelay.start, early)
    zbulk.take(3, zrelay.start)
    lsmall.take(3, only=0)
    lsmall.take(2, only=1)
    xbulk.take(2, xrelay.start)
    lsmall.take(4, only=0)
    lbulk.start(0)
    lsmall.take(3, only=1)
    zbulk.take(4, zrelay.start)
    lsmall.take(4, only=1)
    lbulk.start(1)
    zrelay.take(*zrelay.every())
    xrelay.take(*xrelay.every())
    lbulk.take(1)
    rring.take(1, rrelay.start, late)
    block = mbuf.shape[3]

    @pl.loop(0, nx * nz)
    def _(i):
        at = tile(i, block)
        whi[at], wlo[at] = split(mbuf[0, i // nz, lax.rem(i, nz)])
        shi[at], slo[at] = split(mbuf[1, i // nz, lax.rem(i, nz)])

    def cut(i, j=None):
        return slice(i * unit, (i + 1 if j is None else j) * unit)

    def pair(hi, lo, *at):
        return hi[at], lo[at]

    for i in range(nx):
        for j in range(nx):
            out = 0.0
            top = min(j, i + 1)
            if top > 0:
                out = dot3(pair(whi, wlo, cut(i), cut(0, top)), pair(shi, slo, cut(j), cut(0, top)), NT)
            if j <= i:
                out = out + dot3(pair(whi, wlo, cut(i), cut(j, i + 1)), pair(shi, slo, cut(j, i + 1), cut(j)), NN)
            yhi[cut(i), cut(j)], ylo[cut(i), cut(j)] = split(out)
    for i in range(nx):
        for j in range(i + 1):
            out = dot3(pair(yhi, ylo, cut(i), cut(0, j + 1)), pair(whi, wlo, cut(j), cut(0, j + 1)), NT)
            chi[cut(i), cut(j)], clo[cut(i), cut(j)] = split(out)
    rrelay.take(*rrelay.own())
    rrelay.take(*rring.keys(1))
    far = 2 if ny > 2 else 0

    def near(i):
        return lax.rem(2 * y + nd - 2 + i, nd) if far else i

    @pl.loop(0, nd - far)
    def _(i):
        @pl.when(near(i) != depth)
        def _():
            split_slot(near(i))

    for step in range(2, lbulk.steps + 1):
        lbulk.take(step)
    for c in range(2):
        phi[c, pad:2 * pad], plo[c, pad:2 * pad] = split(lbuf[c])
    def panel_out(at, j):
        out = dot3(pair(phi, plo, 0, at, cut(0, j + 1)), pair(whi, wlo, cut(j), cut(0, j + 1)), NT)
        if j > 0:
            out = out - dot3(pair(phi, plo, 1, at, cut(0, j)), pair(chi, clo, cut(j), cut(0, j)), NT)
        return out - dot3(pair(phi, plo, 1, at, cut(j, nx)), pair(chi, clo, cut(j, nx), cut(j)), NN)

    slab = slice(pad, 2 * pad)
    for j in range(nx):
        qhi[1, :, cut(j)], qlo[1, :, cut(j)] = split(panel_out(slab, j))
        out = dot3(pair(phi, plo, 1, slab, cut(j, nx)), pair(whi, wlo, cut(j, nx), cut(j)), NN)
        qhi[0, :, cut(j)], qlo[0, :, cut(j)] = split(out)

    def slot(i):
        out = dot3(pair(qhi, qlo, 0), pair(rhi, rlo, i, 0), NT)
        ubuf[i, :, 0:rhi.shape[2]] = out + dot3(pair(qhi, qlo, 1), pair(rhi, rlo, i, 1), NT)

    @pl.loop(0, nd - far)
    def _(i):
        slot(near(i))

    for step in range(2, rring.steps + 1):
        rring.take(step, rrelay.start)
    for j in range(nx):
        pbuf[:, cut(j)] = panel_out(slice(0, pad), j)[0:rows]
    p_copy = pltpu.make_async_copy(pbuf, p_out, load.at[1])
    p_copy.start()
    chip = (x * nz + z) * ny + y
    at = tile(chip // 2, 16)
    mine = jnp.concatenate(
        [
            dot3(pair(yhi, ylo, at, cut(0, j + 1)), pair(whi, wlo, cut(j), cut(0, j + 1)), NT)
            for j in range(nx)
        ],
        axis=1,
    )
    mine = jnp.where(lax.rem(chip, 2) == 0, mine[0:8], mine[8:16])
    cbuf[...] = jnp.where(first, mine[0:4], mine[4:8])
    c_copy = pltpu.make_async_copy(cbuf, c_out, load.at[0])
    c_copy.start()
    for step in range(2, rring.steps + 1):
        rrelay.take(*rring.keys(step))
    if far:
        @pl.loop(0, far)
        def _(i):
            at = lax.rem(2 * y + nd // 2 + i, nd)
            split_slot(at)
            slot(at)

    local[6].wait()

    def finish(at):
        update = jnp.concatenate([ubuf[i, at, 0:rows] for i in range(nd)], axis=1)
        tbuf[at, :] = tbuf[at, :] - update

    step = 32
    if rows >= step:
        @pl.loop(0, rows // step)
        def _(i):
            finish(tile(i, step))

    finish(slice(rows // step * step, rows))
    t_copy = pltpu.make_async_copy(tbuf, t_out, load.at[2])
    t_copy.start()

    trade.wait_send()
    for each in (ysmall, xsmall, zsmall, lsmall, rring, zbulk, xbulk, lbulk, rrelay, zrelay, xrelay):
        each.drain()
    @pl.when(on_edge)
    def _():
        for c in range(2):
            for j in range(1, nz):
                zscatter(c, j).wait_send()

    @pl.when(root)
    def _():
        for c in range(2):
            for i in range(1, nx):
                lscatter(c, i).wait_send()

    c_copy.wait()
    p_copy.wait()
    t_copy.wait()


def body(dims, trailing, panel_block, factor_panel, corner_block, corner_inverse):
    nx, nz, ny = dims
    nd = 2 * ny
    rows, width = panel_block.shape
    pad = max(-(-rows // (8 * nx)) * 8 * nx, -(-rows // 16) * 16)
    corner_rows = corner_block.shape[0]
    vmem = pltpu.VMEM
    square = vmem((width, width), BF16)
    any_space = pl.BlockSpec(memory_space=pl.ANY)

    def sems(*counts):
        return [pltpu.SemaphoreType.DMA((n,)) for n in counts for _ in range(2)]

    scratch = [
        vmem((nd, 2, rows, width), F32),
        vmem((nd, 2, pad, width), BF16), vmem((nd, 2, pad, width), BF16),
        vmem((2, pad, width), F32), vmem((2, pad // nx, width), F32), vmem((2, pad, width), F32),
        vmem((2, 2 * pad, width), BF16), vmem((2, 2 * pad, width), BF16),
        vmem((2, nx, nz, 8 * ny, width), F32),
        vmem((2, corner_rows, width), F32), vmem((corner_rows, width), F32),
        *[square] * 8,
        vmem((2, pad, width), BF16), vmem((2, pad, width), BF16),
        vmem((rows, width), F32),
        vmem((nd, pad, 256), F32),
        vmem(trailing.shape, F32),
        vmem((corner_rows, width), F32),
        pltpu.SemaphoreType.DMA((7,)),
        *sems(ny, 4 * ny, nx, 4 * nz, 4 * nz, 4 * nx, 4 * nz, 4 * nx, 4 * ny + 4, 4 * nz + 4, 4 * nx + 4),
        pltpu.SemaphoreType.DMA, pltpu.SemaphoreType.DMA,
        *sems(2 * nx, 2 * nz),
    ]
    return pl.pallas_call(
        functools.partial(kernel, dims),
        out_shape=(
            jax.ShapeDtypeStruct(trailing.shape, F32),
            jax.ShapeDtypeStruct(panel_block.shape, F32),
            jax.ShapeDtypeStruct(corner_block.shape, F32),
        ),
        in_specs=[any_space] * 5,
        out_specs=(any_space,) * 3,
        scratch_shapes=scratch,
        compiler_params=pltpu.CompilerParams(
            collective_id=0, has_side_effects=True, vmem_limit_bytes=67_000_000
        ),
        name="panel_step",
    )(trailing, panel_block, factor_panel, corner_block, corner_inverse)


def solution(mesh):
    dims = (mesh.shape["row"], mesh.shape["col"], mesh.shape["depth"] // 2)
    columns = P("depth", ("row", "col"))
    spread = P(("row", "col", "depth"), None)
    return jax.shard_map(
        functools.partial(body, dims),
        mesh=mesh,
        in_specs=(columns, spread, spread, spread, spread),
        out_specs=(columns, spread, spread),
        check_vma=False,
    )
```

```python
import functools

import jax
import jax.numpy as jnp
from jax import lax
from jax.experimental import pallas as pl
from jax.experimental.pallas import tpu as pltpu
from jax.sharding import PartitionSpec as P

F32, BF16 = jnp.float32, jnp.bfloat16
MESH = pl.DeviceIdType.MESH
NN = (((1,), (0,)), ((), ()))
NT = (((1,), (1,)), ((), ()))


def split(x):
    hi = x.astype(BF16)
    return hi, (x - hi.astype(F32)).astype(BF16)


def dot3(a, b, dims):
    (ah, al), (bh, bl) = a, b
    dot = functools.partial(lax.dot_general, dimension_numbers=dims, preferred_element_type=F32)
    return dot(ah, bh) + dot(ah, bl) + dot(al, bh)


def remote(src, dst, send, recv, device):
    return pltpu.make_async_remote_copy(
        src_ref=src, dst_ref=dst, send_sem=send, recv_sem=recv, device_id=device, device_id_type=MESH
    )


class Direct:
    def __init__(self, n, me, device, block, send, recv):
        self.n, self.me, self.device, self.block, self.send, self.recv = n, me, device, block, send, recv

    def copy(self, j, incoming=False):
        ref = self.block(lax.rem(self.me + self.n - j, self.n) if incoming else self.me)
        return remote(ref, ref, self.send.at[j], self.recv.at[j], self.device(lax.rem(self.me + j, self.n)))

    def start(self):
        for j in sorted(range(1, self.n), key=lambda j: -min(j, self.n - j)):
            self.copy(j).start()

    def take(self):
        for j in range(1, self.n):
            self.copy(j, incoming=True).wait_recv()

    def drain(self):
        for j in range(1, self.n):
            self.copy(j).wait_send()


class Ring:
    def __init__(self, n, me, device, block, counts, send, recv):
        self.n, self.me, self.device, self.block, self.counts = n, me, device, block, counts
        self.send, self.recv, self.steps = send, recv, n // 2

    def keys(self, step):
        out = []
        for at in range(2):
            for way in range(2):
                chunk = at if way == 0 else 1 - at
                if step < self.steps or chunk == way:
                    out += [(way, step, chunk, piece) for piece in range(self.counts[chunk])]
        return out

    def index(self, way, step, chunk, piece):
        return ((way * self.steps + step - 1) * 2 + chunk) * 2 + piece

    def origin(self, way, hops):
        return lax.rem(self.me - (hops if way == 0 else -hops) + self.n, self.n)

    def copy(self, way, step, chunk, piece, incoming=False):
        ref = self.block(self.origin(way, step if incoming else step - 1), chunk, piece)
        target = lax.rem(self.me + (1 if way == 0 else -1) + self.n, self.n)
        k = self.index(way, step, chunk, piece)
        return remote(ref, ref, self.send.at[k], self.recv.at[k], self.device(target))

    def start(self):
        for key in self.keys(1):
            self.copy(*key).start()

    def take(self, step, then=None, keys=None):
        for key in self.keys(step) if keys is None else keys:
            way, step, chunk, piece = key
            self.copy(*key, incoming=True).wait_recv()
            if step < self.steps and (step + 1 < self.steps or chunk == way):
                self.copy(way, step + 1, chunk, piece).start()
            if then is not None:
                then(*key)

    def drain(self):
        for step in range(1, self.steps + 1):
            for key in self.keys(step):
                self.copy(*key).wait_send()


class Relay:
    def __init__(self, ring, theirs, device, send, recv):
        self.ring, self.theirs, self.device, self.send, self.recv = ring, theirs, device, send, recv

    def own(self):
        counts = self.ring.counts
        return [(0, 0, chunk, piece) for chunk in range(2) for piece in range(counts[chunk])]

    def copy(self, way, step, chunk, piece, incoming=False):
        ref = (self.theirs if incoming else self.ring.block)(self.ring.origin(way, step), chunk, piece)
        k = chunk * 2 + piece if step == 0 else 4 + self.ring.index(way, step, chunk, piece)
        return remote(ref, ref, self.send.at[k], self.recv.at[k], self.device)

    def start(self, *key):
        self.copy(*key).start()

    def start_own(self):
        for key in self.own():
            self.copy(*key).start()

    def take(self, *keys):
        for key in keys:
            self.copy(*key, incoming=True).wait_recv()

    def every(self):
        return self.own() + [key for step in range(1, self.ring.steps + 1) for key in self.ring.keys(step)]

    def drain(self):
        for key in self.every():
            self.copy(*key).wait_send()


def kernel(
    dims, trailing, a_in, f_in, s_in, w_in, t_out, p_out, c_out,
    rbuf, rhi, rlo, lsrc, lbuf, phi, plo, mbuf, rows4, swap, whi, wlo, shi, slo, yhi, ylo, chi, clo,
    qhi, qlo, pbuf, ubuf, tbuf, cbuf,
    load, ysend, yrecv, rsend, rrecv, xs_send, xs_recv, zs_send, zs_recv, zb_send, zb_recv, xb_send, xb_recv,
    ls_send, ls_recv, lb_send, lb_recv, dr_send, dr_recv, dz_send, dz_recv, dx_send, dx_recv,
    sw_send, sw_recv, lx_send, lx_recv, lz_send, lz_recv,
):
    nx, nz, ny = dims
    nd = 2 * ny
    rows, width = a_in.shape
    whole = rows // 8 * 8
    x, z, depth = lax.axis_index("row"), lax.axis_index("col"), lax.axis_index("depth")
    y, core = depth // 2, lax.rem(depth, 2)
    pad = lbuf.shape[1]
    lx, lz = pad // nx, width // nz
    unit, half = width // nx, width // 2
    on_edge, on_side = z == 0, x == 0
    root = jnp.logical_and(on_edge, on_side)
    partner = {"depth": y * 2 + 1 - core}

    def on_x(i):
        return {"row": i}

    def on_y(i):
        return {"depth": i * 2 + core}

    def on_z(i):
        return {"col": i}

    def tile(i, size):
        return pl.ds(pl.multiple_of(i * size, size), size)

    def line(c, i):
        return lsrc.at[c, tile(i, lx)], lbuf.at[c, tile(i, lx)]

    def lscatter(c, i):
        src, dst = line(c, i)
        return remote(src, dst, lx_send.at[c * nx + i], lx_recv.at[c], on_x(i))

    def part(c, j):
        return lbuf.at[c, tile(x, lx), tile(j, lz)]

    def zscatter(c, j):
        return remote(part(c, j), part(c, j), lz_send.at[c * nz + j], lz_recv.at[c], on_z(j))

    def lsmall(c, j, incoming=False):
        ref = part(c, lax.rem(z + nz - j, nz) if incoming else z)
        return remote(ref, ref, ls_send.at[c * nz + j], ls_recv.at[c * nz + j], on_z(lax.rem(z + j, nz)))

    def lsmall_sends(c, act):
        for j in range(1, nz):
            @pl.when(lax.rem(z + j, nz) != 0)
            def _():
                act(lsmall(c, j))

    def edge(c):
        @pl.when(on_edge)
        def _():
            @pl.when(jnp.logical_not(on_side))
            def _():
                lscatter(c, x).wait_recv()

            for j in range(1, nz):
                zscatter(c, j).start()
            lsmall_sends(c, lambda copy: copy.start())

    def inner(c):
        @pl.when(jnp.logical_not(on_edge))
        def _():
            zscatter(c, z).wait_recv()
            lsmall_sends(c, lambda copy: copy.start())

    def gathered(c):
        @pl.when(jnp.logical_not(on_edge))
        def _():
            for j in range(1, nz):
                lsmall(c, j, incoming=True).wait_recv()

        for key in lbulk.keys(1):
            if key[2] == c:
                lbulk.copy(*key).start()

    lbulk = Ring(nx, x, on_x, lambda i, chunk, piece: lbuf.at[chunk, tile(i, lx)], (1, 1), lb_send, lb_recv)

    loads = [
        (w_in, rows4.at[0]),
        (s_in, rows4.at[1]),
        (a_in, rbuf.at[depth, 0]),
        (f_in, rbuf.at[depth, 1]),
        (a_in.at[pl.ds(0, whole)], lsrc.at[0, pl.ds(0, whole)]),
        (f_in.at[pl.ds(0, whole)], lsrc.at[1, pl.ds(0, whole)]),
        (trailing, tbuf),
    ]
    local = [pltpu.make_async_copy(src, dst, load.at[i]) for i, (src, dst) in enumerate(loads)]
    for copy in local:
        copy.start()

    barrier = pltpu.get_barrier_semaphore()
    peers = [partner]
    peers += [on_y(lax.rem(y + j, ny)) for j in range(1, ny)]
    peers += [on_x(lax.rem(x + j, nx)) for j in range(1, nx)]
    peers += [on_z(lax.rem(z + j, nz)) for j in range(1, nz)]
    for peer in peers:
        pl.semaphore_signal(barrier, inc=1, device_id=peer, device_id_type=MESH)

    for copy in local[:6]:
        copy.wait()
    lsrc[:, whole:rows] = rbuf[depth, :, whole:rows]

    pl.semaphore_wait(barrier, len(peers))

    trade = remote(rows4.at[1 - core], swap, sw_send, sw_recv, partner)
    trade.start()

    def panel(who):
        return lambda i, chunk, piece: rbuf.at[i * 2 + who, chunk, :, pl.ds(piece * half, half)]

    rring = Ring(ny, y, on_y, panel(core), (2, 2), rsend, rrecv)
    rrelay = Relay(rring, panel(1 - core), partner, dr_send, dr_recv)

    def myrow(i):
        return mbuf.at[core, x, z, tile(i, 8)]

    ysmall = Direct(ny, y, on_y, myrow, ysend, yrecv)

    @pl.when(root)
    def _():
        for c in range(2):
            for i in range(1, nx):
                lscatter(c, i).start()
        lbuf[:, 0:lx] = lsrc[:, 0:lx]

    trade.wait_recv()
    own, got = rows4[core], swap[...]
    first = core == 0
    mbuf[core, x, z, tile(y, 8), :] = jnp.concatenate(
        [jnp.where(first, own, got), jnp.where(first, got, own)], axis=0
    )
    ysmall.start()
    rring.start()

    def split_slot(i):
        for c in range(2):
            rhi[i, c, 0:rows], rlo[i, c, 0:rows] = split(rbuf[i, c])

    split_slot(depth)
    for c in range(2):
        phi[c, 0:rows] = rhi[depth, c, 0:rows]
        plo[c, 0:rows] = rlo[depth, c, 0:rows]

    rest = pl.ds(unit, width - unit)
    xsmall = Direct(nx, x, on_x, lambda i: mbuf.at[core, i, z, :, rest], xs_send, xs_recv)
    zsmall = Direct(nz, z, on_z, lambda i: mbuf.at[core, x, i, :, pl.ds(0, unit)], zs_send, zs_recv)
    layout = ([nx - 1], list(range(nx - 2, 0, -1)))

    def zblock(who):
        def block(i, chunk, piece):
            at = layout[chunk][piece]
            return mbuf.at[who, at, i, :, pl.ds(unit, at * unit)]
        return block

    def xblock(who):
        return lambda i, chunk, piece: mbuf.at[who, i, pl.ds(chunk * (nz // 2), nz // 2), :, pl.ds(0, unit)]

    zbulk = Ring(nz, z, on_z, zblock(core), tuple(len(part) for part in layout), zb_send, zb_recv)
    zrelay = Relay(zbulk, zblock(1 - core), partner, dz_send, dz_recv)
    xbulk = Ring(nx, x, on_x, xblock(core), (1, 1), xb_send, xb_recv)
    xrelay = Relay(xbulk, xblock(1 - core), partner, dx_send, dx_recv)

    ysmall.take()
    xsmall.start()
    zsmall.start()
    rrelay.start_own()
    edge(0)
    xsmall.take()
    zbulk.start()
    zrelay.start_own()
    zsmall.take()
    xbulk.start()
    xrelay.start_own()
    inner(0)
    edge(1)
    zbulk.take(1, zrelay.start)
    inner(1)
    if zbulk.steps > 1:
        zbulk.take(2, zrelay.start)
    xbulk.take(1, xrelay.start)
    early = [key for key in rring.keys(1) if key[2] == key[0]]
    late = [key for key in rring.keys(1) if key[2] != key[0]]
    rring.take(1, rrelay.start, early)
    gathered(0)
    if zbulk.steps > 2:
        zbulk.take(3, zrelay.start)
    for step in range(2, xbulk.steps + 1):
        xbulk.take(step, xrelay.start)
    gathered(1)
    for step in range(4, zbulk.steps + 1):
        zbulk.take(step, zrelay.start)
    zrelay.take(*zrelay.every())
    xrelay.take(*xrelay.every())
    rring.take(1, rrelay.start, late)
    block = mbuf.shape[3]

    @pl.loop(0, nx * nz)
    def _(i):
        at = tile(i, block)
        whi[at], wlo[at] = split(mbuf[0, i // nz, lax.rem(i, nz)])
        shi[at], slo[at] = split(mbuf[1, i // nz, lax.rem(i, nz)])

    def cut(i, j=None):
        return slice(i * unit, (i + 1 if j is None else j) * unit)

    def pair(hi, lo, *at):
        return hi[at], lo[at]

    for i in range(nx):
        for j in range(nx):
            out = 0.0
            top = min(j, i + 1)
            if top > 0:
                out = dot3(pair(whi, wlo, cut(i), cut(0, top)), pair(shi, slo, cut(j), cut(0, top)), NT)
            if j <= i:
                out = out + dot3(pair(whi, wlo, cut(i), cut(j, i + 1)), pair(shi, slo, cut(j, i + 1), cut(j)), NN)
            yhi[cut(i), cut(j)], ylo[cut(i), cut(j)] = split(out)
    lbulk.take(1)
    for i in range(nx):
        for j in range(i + 1):
            out = dot3(pair(yhi, ylo, cut(i), cut(0, j + 1)), pair(whi, wlo, cut(j), cut(0, j + 1)), NT)
            chi[cut(i), cut(j)], clo[cut(i), cut(j)] = split(out)
    rrelay.take(*rrelay.own())
    rrelay.take(*rring.keys(1))
    far = 2 if ny > 2 else 0

    def near(i):
        return lax.rem(2 * y + nd - 2 + i, nd) if far else i

    @pl.loop(0, nd - far)
    def _(i):
        @pl.when(near(i) != depth)
        def _():
            split_slot(near(i))

    for step in range(2, lbulk.steps + 1):
        lbulk.take(step)
    for c in range(2):
        phi[c, pad:2 * pad], plo[c, pad:2 * pad] = split(lbuf[c])
    def panel_out(at, j):
        out = dot3(pair(phi, plo, 0, at, cut(0, j + 1)), pair(whi, wlo, cut(j), cut(0, j + 1)), NT)
        if j > 0:
            out = out - dot3(pair(phi, plo, 1, at, cut(0, j)), pair(chi, clo, cut(j), cut(0, j)), NT)
        return out - dot3(pair(phi, plo, 1, at, cut(j, nx)), pair(chi, clo, cut(j, nx), cut(j)), NN)

    slab = slice(pad, 2 * pad)
    for j in range(nx):
        qhi[1, :, cut(j)], qlo[1, :, cut(j)] = split(panel_out(slab, j))
        out = dot3(pair(phi, plo, 1, slab, cut(j, nx)), pair(whi, wlo, cut(j, nx), cut(j)), NN)
        qhi[0, :, cut(j)], qlo[0, :, cut(j)] = split(out)

    def slot(i):
        out = dot3(pair(qhi, qlo, 0), pair(rhi, rlo, i, 0), NT)
        ubuf[i, :, 0:rhi.shape[2]] = out + dot3(pair(qhi, qlo, 1), pair(rhi, rlo, i, 1), NT)

    @pl.loop(0, nd - far)
    def _(i):
        slot(near(i))

    for step in range(2, rring.steps + 1):
        rring.take(step, rrelay.start)
    for j in range(nx):
        pbuf[:, cut(j)] = panel_out(slice(0, pad), j)[0:rows]
    p_copy = pltpu.make_async_copy(pbuf, p_out, load.at[1])
    p_copy.start()
    chip = (x * nz + z) * ny + y
    at = tile(chip // 2, 16)
    mine = jnp.concatenate(
        [
            dot3(pair(yhi, ylo, at, cut(0, j + 1)), pair(whi, wlo, cut(j), cut(0, j + 1)), NT)
            for j in range(nx)
        ],
        axis=1,
    )
    mine = jnp.where(lax.rem(chip, 2) == 0, mine[0:8], mine[8:16])
    cbuf[...] = jnp.where(first, mine[0:4], mine[4:8])
    c_copy = pltpu.make_async_copy(cbuf, c_out, load.at[0])
    c_copy.start()
    for step in range(2, rring.steps + 1):
        rrelay.take(*rring.keys(step))
    if far:
        @pl.loop(0, far)
        def _(i):
            at = lax.rem(2 * y + nd // 2 + i, nd)
            split_slot(at)
            slot(at)

    local[6].wait()

    def finish(at):
        update = jnp.concatenate([ubuf[i, at, 0:rows] for i in range(nd)], axis=1)
        tbuf[at, :] = tbuf[at, :] - update

    step = 32
    if rows >= step:
        @pl.loop(0, rows // step)
        def _(i):
            finish(tile(i, step))

    finish(slice(rows // step * step, rows))
    t_copy = pltpu.make_async_copy(tbuf, t_out, load.at[2])
    t_copy.start()

    trade.wait_send()
    for each in (ysmall, xsmall, zsmall, rring, zbulk, xbulk, lbulk, rrelay, zrelay, xrelay):
        each.drain()
    for c in range(2):
        lsmall_sends(c, lambda copy: copy.wait_send())

    @pl.when(on_edge)
    def _():
        for c in range(2):
            for j in range(1, nz):
                zscatter(c, j).wait_send()

    @pl.when(root)
    def _():
        for c in range(2):
            for i in range(1, nx):
                lscatter(c, i).wait_send()

    c_copy.wait()
    p_copy.wait()
    t_copy.wait()


def body(dims, trailing, panel_block, factor_panel, corner_block, corner_inverse):
    nx, nz, ny = dims
    nd = 2 * ny
    rows, width = panel_block.shape
    pad = max(-(-rows // (8 * nx)) * 8 * nx, -(-rows // 16) * 16)
    corner_rows = corner_block.shape[0]
    vmem = pltpu.VMEM
    square = vmem((width, width), BF16)
    any_space = pl.BlockSpec(memory_space=pl.ANY)

    def sems(*counts):
        return [pltpu.SemaphoreType.DMA((n,)) for n in counts for _ in range(2)]

    scratch = [
        vmem((nd, 2, rows, width), F32),
        vmem((nd, 2, pad, width), BF16), vmem((nd, 2, pad, width), BF16),
        vmem((2, pad, width), F32), vmem((2, pad, width), F32),
        vmem((2, 2 * pad, width), BF16), vmem((2, 2 * pad, width), BF16),
        vmem((2, nx, nz, 8 * ny, width), F32),
        vmem((2, corner_rows, width), F32), vmem((corner_rows, width), F32),
        *[square] * 8,
        vmem((2, pad, width), BF16), vmem((2, pad, width), BF16),
        vmem((rows, width), F32),
        vmem((nd, pad, 256), F32),
        vmem(trailing.shape, F32),
        vmem((corner_rows, width), F32),
        pltpu.SemaphoreType.DMA((7,)),
        *sems(ny, 4 * ny, nx, nz, 4 * nz, 4 * nx, 2 * nz, 4 * nx, 4 * ny + 4, 4 * nz + 4, 4 * nx + 4),
        pltpu.SemaphoreType.DMA, pltpu.SemaphoreType.DMA,
        *sems(2 * nx, 2 * nz),
    ]
    return pl.pallas_call(
        functools.partial(kernel, dims),
        out_shape=(
            jax.ShapeDtypeStruct(trailing.shape, F32),
            jax.ShapeDtypeStruct(panel_block.shape, F32),
            jax.ShapeDtypeStruct(corner_block.shape, F32),
        ),
        in_specs=[any_space] * 5,
        out_specs=(any_space,) * 3,
        scratch_shapes=scratch,
        compiler_params=pltpu.CompilerParams(
            collective_id=0, has_side_effects=True, vmem_limit_bytes=67_000_000
        ),
        name="panel_step",
    )(trailing, panel_block, factor_panel, corner_block, corner_inverse)


def solution(mesh):
    dims = (mesh.shape["row"], mesh.shape["col"], mesh.shape["depth"] // 2)
    columns = P("depth", ("row", "col"))
    spread = P(("row", "col", "depth"), None)
    return jax.shard_map(
        functools.partial(body, dims),
        mesh=mesh,
        in_specs=(columns, spread, spread, spread, spread),
        out_specs=(columns, spread, spread),
        check_vma=False,
    )
```

```python
import functools

import jax
import jax.numpy as jnp
from jax import lax
from jax.experimental import pallas as pl
from jax.experimental.pallas import tpu as pltpu
from jax.sharding import PartitionSpec as P

F32, BF16 = jnp.float32, jnp.bfloat16
MESH = pl.DeviceIdType.MESH
NN = (((1,), (0,)), ((), ()))
NT = (((1,), (1,)), ((), ()))


def split(x):
    hi = x.astype(BF16)
    return hi, (x - hi.astype(F32)).astype(BF16)


def dot3(a, b, dims):
    (ah, al), (bh, bl) = a, b
    dot = functools.partial(lax.dot_general, dimension_numbers=dims, preferred_element_type=F32)
    return dot(ah, bh) + dot(ah, bl) + dot(al, bh)


def remote(src, dst, send, recv, device):
    return pltpu.make_async_remote_copy(
        src_ref=src, dst_ref=dst, send_sem=send, recv_sem=recv, device_id=device, device_id_type=MESH
    )


class Direct:
    def __init__(self, n, me, device, block, send, recv):
        self.n, self.me, self.device, self.block, self.send, self.recv = n, me, device, block, send, recv

    def copy(self, j, incoming=False):
        ref = self.block(lax.rem(self.me + self.n - j, self.n) if incoming else self.me)
        return remote(ref, ref, self.send.at[j], self.recv.at[j], self.device(lax.rem(self.me + j, self.n)))

    def start(self):
        for j in sorted(range(1, self.n), key=lambda j: -min(j, self.n - j)):
            self.copy(j).start()

    def take(self):
        for j in range(1, self.n):
            self.copy(j, incoming=True).wait_recv()

    def drain(self):
        for j in range(1, self.n):
            self.copy(j).wait_send()


class Ring:
    def __init__(self, n, me, device, block, counts, send, recv):
        self.n, self.me, self.device, self.block, self.counts = n, me, device, block, counts
        self.send, self.recv, self.steps = send, recv, n // 2

    def keys(self, step):
        out = []
        for at in range(2):
            for way in range(2):
                chunk = at if way == 0 else 1 - at
                if step < self.steps or chunk == way:
                    out += [(way, step, chunk, piece) for piece in range(self.counts[chunk])]
        return out

    def index(self, way, step, chunk, piece):
        return ((way * self.steps + step - 1) * 2 + chunk) * 2 + piece

    def origin(self, way, hops):
        return lax.rem(self.me - (hops if way == 0 else -hops) + self.n, self.n)

    def copy(self, way, step, chunk, piece, incoming=False):
        ref = self.block(self.origin(way, step if incoming else step - 1), chunk, piece)
        target = lax.rem(self.me + (1 if way == 0 else -1) + self.n, self.n)
        k = self.index(way, step, chunk, piece)
        return remote(ref, ref, self.send.at[k], self.recv.at[k], self.device(target))

    def start(self):
        for key in self.keys(1):
            self.copy(*key).start()

    def take(self, step, then=None, keys=None):
        for key in self.keys(step) if keys is None else keys:
            way, step, chunk, piece = key
            self.copy(*key, incoming=True).wait_recv()
            if step < self.steps and (step + 1 < self.steps or chunk == way):
                self.copy(way, step + 1, chunk, piece).start()
            if then is not None:
                then(*key)

    def drain(self):
        for step in range(1, self.steps + 1):
            for key in self.keys(step):
                self.copy(*key).wait_send()


class Relay:
    def __init__(self, ring, theirs, device, send, recv):
        self.ring, self.theirs, self.device, self.send, self.recv = ring, theirs, device, send, recv

    def own(self):
        counts = self.ring.counts
        return [(0, 0, chunk, piece) for chunk in range(2) for piece in range(counts[chunk])]

    def copy(self, way, step, chunk, piece, incoming=False):
        ref = (self.theirs if incoming else self.ring.block)(self.ring.origin(way, step), chunk, piece)
        k = chunk * 2 + piece if step == 0 else 4 + self.ring.index(way, step, chunk, piece)
        return remote(ref, ref, self.send.at[k], self.recv.at[k], self.device)

    def start(self, *key):
        self.copy(*key).start()

    def start_own(self):
        for key in self.own():
            self.copy(*key).start()

    def take(self, *keys):
        for key in keys:
            self.copy(*key, incoming=True).wait_recv()

    def every(self):
        return self.own() + [key for step in range(1, self.ring.steps + 1) for key in self.ring.keys(step)]

    def drain(self):
        for key in self.every():
            self.copy(*key).wait_send()


def kernel(
    dims, trailing, a_in, f_in, s_in, w_in, t_out, p_out, c_out,
    rbuf, rhi, rlo, lsrc, lbuf, phi, plo, mbuf, rows4, swap, whi, wlo, shi, slo, yhi, ylo, chi, clo,
    qhi, qlo, pbuf, ubuf, tbuf, cbuf,
    load, ysend, yrecv, rsend, rrecv, xs_send, xs_recv, zs_send, zs_recv, zb_send, zb_recv, xb_send, xb_recv,
    ls_send, ls_recv, lb_send, lb_recv, dr_send, dr_recv, dz_send, dz_recv, dx_send, dx_recv,
    sw_send, sw_recv, lx_send, lx_recv, lz_send, lz_recv,
):
    nx, nz, ny = dims
    nd = 2 * ny
    rows, width = a_in.shape
    whole = rows // 8 * 8
    x, z, depth = lax.axis_index("row"), lax.axis_index("col"), lax.axis_index("depth")
    y, core = depth // 2, lax.rem(depth, 2)
    pad = lbuf.shape[1]
    lx, lz = pad // nx, width // nz
    unit, half = width // nx, width // 2
    on_edge, on_side = z == 0, x == 0
    root = jnp.logical_and(on_edge, on_side)
    partner = {"depth": y * 2 + 1 - core}

    def on_x(i):
        return {"row": i}

    def on_y(i):
        return {"depth": i * 2 + core}

    def on_z(i):
        return {"col": i}

    def tile(i, size):
        return pl.ds(pl.multiple_of(i * size, size), size)

    def line(c, i):
        return lsrc.at[c, tile(i, lx)], lbuf.at[c, tile(i, lx)]

    def lscatter(c, i):
        src, dst = line(c, i)
        return remote(src, dst, lx_send.at[c * nx + i], lx_recv.at[c], on_x(i))

    def part(c, j):
        return lbuf.at[c, tile(x, lx), tile(j, lz)]

    def zscatter(c, j):
        return remote(part(c, j), part(c, j), lz_send.at[c * nz + j], lz_recv.at[c], on_z(j))

    def lsmall(c, j, incoming=False):
        ref = part(c, lax.rem(z + nz - j, nz) if incoming else z)
        return remote(ref, ref, ls_send.at[c * nz + j], ls_recv.at[c * nz + j], on_z(lax.rem(z + j, nz)))

    def lsmall_sends(c, act):
        for j in range(1, nz):
            @pl.when(lax.rem(z + j, nz) != 0)
            def _():
                act(lsmall(c, j))

    def edge(c):
        @pl.when(on_edge)
        def _():
            @pl.when(jnp.logical_not(on_side))
            def _():
                lscatter(c, x).wait_recv()

            for j in range(1, nz):
                zscatter(c, j).start()
            lsmall_sends(c, lambda copy: copy.start())

    def inner(c):
        @pl.when(jnp.logical_not(on_edge))
        def _():
            zscatter(c, z).wait_recv()
            lsmall_sends(c, lambda copy: copy.start())

    def gathered(c):
        @pl.when(jnp.logical_not(on_edge))
        def _():
            for j in range(1, nz):
                lsmall(c, j, incoming=True).wait_recv()

        for key in lbulk.keys(1):
            if key[2] == c:
                lbulk.copy(*key).start()

    lbulk = Ring(nx, x, on_x, lambda i, chunk, piece: lbuf.at[chunk, tile(i, lx)], (1, 1), lb_send, lb_recv)

    loads = [
        (w_in, rows4.at[0]),
        (s_in, rows4.at[1]),
        (a_in, rbuf.at[depth, 0]),
        (f_in, rbuf.at[depth, 1]),
        (a_in.at[pl.ds(0, whole)], lsrc.at[0, pl.ds(0, whole)]),
        (f_in.at[pl.ds(0, whole)], lsrc.at[1, pl.ds(0, whole)]),
        (trailing, tbuf),
    ]
    local = [pltpu.make_async_copy(src, dst, load.at[i]) for i, (src, dst) in enumerate(loads)]
    for copy in local:
        copy.start()

    barrier = pltpu.get_barrier_semaphore()
    peers = [partner]
    peers += [on_y(lax.rem(y + j, ny)) for j in range(1, ny)]
    peers += [on_x(lax.rem(x + j, nx)) for j in range(1, nx)]
    peers += [on_z(lax.rem(z + j, nz)) for j in range(1, nz)]
    for peer in peers:
        pl.semaphore_signal(barrier, inc=1, device_id=peer, device_id_type=MESH)

    for copy in local[:6]:
        copy.wait()
    lsrc[:, whole:rows] = rbuf[depth, :, whole:rows]

    pl.semaphore_wait(barrier, len(peers))

    trade = remote(rows4.at[1 - core], swap, sw_send, sw_recv, partner)
    trade.start()

    def panel(who):
        return lambda i, chunk, piece: rbuf.at[i * 2 + who, chunk, :, pl.ds(piece * half, half)]

    rring = Ring(ny, y, on_y, panel(core), (2, 2), rsend, rrecv)
    rrelay = Relay(rring, panel(1 - core), partner, dr_send, dr_recv)

    def myrow(i):
        return mbuf.at[core, x, z, tile(i, 8)]

    ysmall = Direct(ny, y, on_y, myrow, ysend, yrecv)

    @pl.when(root)
    def _():
        for c in range(2):
            for i in range(1, nx):
                lscatter(c, i).start()
        lbuf[:, 0:lx] = lsrc[:, 0:lx]

    trade.wait_recv()
    own, got = rows4[core], swap[...]
    first = core == 0
    mbuf[core, x, z, tile(y, 8), :] = jnp.concatenate(
        [jnp.where(first, own, got), jnp.where(first, got, own)], axis=0
    )
    ysmall.start()
    rring.start()

    def split_slot(i):
        for c in range(2):
            rhi[i, c, 0:rows], rlo[i, c, 0:rows] = split(rbuf[i, c])

    split_slot(depth)
    for c in range(2):
        phi[c, 0:rows] = rhi[depth, c, 0:rows]
        plo[c, 0:rows] = rlo[depth, c, 0:rows]

    rest = pl.ds(unit, width - unit)
    xsmall = Direct(nx, x, on_x, lambda i: mbuf.at[core, i, z, :, rest], xs_send, xs_recv)
    zsmall = Direct(nz, z, on_z, lambda i: mbuf.at[core, x, i, :, pl.ds(0, unit)], zs_send, zs_recv)
    layout = ([nx - 1], list(range(nx - 2, 0, -1)))

    def zblock(who):
        def block(i, chunk, piece):
            at = layout[chunk][piece]
            return mbuf.at[who, at, i, :, pl.ds(unit, at * unit)]
        return block

    def xblock(who):
        return lambda i, chunk, piece: mbuf.at[who, i, pl.ds(chunk * (nz // 2), nz // 2), :, pl.ds(0, unit)]

    zbulk = Ring(nz, z, on_z, zblock(core), tuple(len(part) for part in layout), zb_send, zb_recv)
    zrelay = Relay(zbulk, zblock(1 - core), partner, dz_send, dz_recv)
    xbulk = Ring(nx, x, on_x, xblock(core), (1, 1), xb_send, xb_recv)
    xrelay = Relay(xbulk, xblock(1 - core), partner, dx_send, dx_recv)

    ysmall.take()
    xsmall.start()
    zsmall.start()
    rrelay.start_own()
    edge(0)
    xsmall.take()
    zbulk.start()
    zrelay.start_own()
    zsmall.take()
    xbulk.start()
    xrelay.start_own()
    inner(0)
    edge(1)
    zbulk.take(1, zrelay.start)
    inner(1)
    if zbulk.steps > 1:
        zbulk.take(2, zrelay.start)
    xbulk.take(1, xrelay.start)
    early = [key for key in rring.keys(1) if key[2] == key[0]]
    late = [key for key in rring.keys(1) if key[2] != key[0]]
    rring.take(1, rrelay.start, early)
    gathered(0)
    if zbulk.steps > 2:
        zbulk.take(3, zrelay.start)
    for step in range(2, xbulk.steps + 1):
        xbulk.take(step, xrelay.start)
    gathered(1)
    for step in range(4, zbulk.steps + 1):
        zbulk.take(step, zrelay.start)
    zrelay.take(*zrelay.every())
    xrelay.take(*xrelay.every())
    rring.take(1, rrelay.start, late)
    block = mbuf.shape[3]

    @pl.loop(0, nx * nz)
    def _(i):
        at = tile(i, block)
        whi[at], wlo[at] = split(mbuf[0, i // nz, lax.rem(i, nz)])
        shi[at], slo[at] = split(mbuf[1, i // nz, lax.rem(i, nz)])

    def cut(i, j=None):
        return slice(i * unit, (i + 1 if j is None else j) * unit)

    def pair(hi, lo, *at):
        return hi[at], lo[at]

    for i in range(nx):
        for j in range(nx):
            out = 0.0
            top = min(j, i + 1)
            if top > 0:
                out = dot3(pair(whi, wlo, cut(i), cut(0, top)), pair(shi, slo, cut(j), cut(0, top)), NT)
            if j <= i:
                out = out + dot3(pair(whi, wlo, cut(i), cut(j, i + 1)), pair(shi, slo, cut(j, i + 1), cut(j)), NN)
            yhi[cut(i), cut(j)], ylo[cut(i), cut(j)] = split(out)
    lbulk.take(1)
    for i in range(nx):
        for j in range(i + 1):
            out = dot3(pair(yhi, ylo, cut(i), cut(0, j + 1)), pair(whi, wlo, cut(j), cut(0, j + 1)), NT)
            chi[cut(i), cut(j)], clo[cut(i), cut(j)] = split(out)
    rrelay.take(*rrelay.own())
    rrelay.take(*rring.keys(1))
    far = 2 if ny > 2 else 0

    def near(i):
        return lax.rem(2 * y + nd - 2 + i, nd) if far else i

    @pl.loop(0, nd - far)
    def _(i):
        @pl.when(near(i) != depth)
        def _():
            split_slot(near(i))

    def panel_out(at, j):
        out = dot3(pair(phi, plo, 0, at, cut(0, j + 1)), pair(whi, wlo, cut(j), cut(0, j + 1)), NT)
        if j > 0:
            out = out - dot3(pair(phi, plo, 1, at, cut(0, j)), pair(chi, clo, cut(j), cut(0, j)), NT)
        return out - dot3(pair(phi, plo, 1, at, cut(j, nx)), pair(chi, clo, cut(j, nx), cut(j)), NN)

    for j in range(nx):
        pbuf[:, cut(j)] = panel_out(slice(0, pad), j)[0:rows]
    p_copy = pltpu.make_async_copy(pbuf, p_out, load.at[1])
    p_copy.start()
    chip = (x * nz + z) * ny + y
    at = tile(chip // 2, 16)
    mine = jnp.concatenate(
        [
            dot3(pair(yhi, ylo, at, cut(0, j + 1)), pair(whi, wlo, cut(j), cut(0, j + 1)), NT)
            for j in range(nx)
        ],
        axis=1,
    )
    mine = jnp.where(lax.rem(chip, 2) == 0, mine[0:8], mine[8:16])
    cbuf[...] = jnp.where(first, mine[0:4], mine[4:8])
    c_copy = pltpu.make_async_copy(cbuf, c_out, load.at[0])
    c_copy.start()
    for step in range(2, lbulk.steps + 1):
        lbulk.take(step)
    for c in range(2):
        phi[c, pad:2 * pad], plo[c, pad:2 * pad] = split(lbuf[c])
    slab = slice(pad, 2 * pad)
    for j in range(nx):
        qhi[1, :, cut(j)], qlo[1, :, cut(j)] = split(panel_out(slab, j))
        out = dot3(pair(phi, plo, 1, slab, cut(j, nx)), pair(whi, wlo, cut(j, nx), cut(j)), NN)
        qhi[0, :, cut(j)], qlo[0, :, cut(j)] = split(out)

    for step in range(2, rring.steps + 1):
        rring.take(step, rrelay.start)
    def slot(i):
        out = dot3(pair(qhi, qlo, 0), pair(rhi, rlo, i, 0), NT)
        ubuf[i, :, 0:rhi.shape[2]] = out + dot3(pair(qhi, qlo, 1), pair(rhi, rlo, i, 1), NT)

    @pl.loop(0, nd - far)
    def _(i):
        slot(near(i))

    for step in range(2, rring.steps + 1):
        rrelay.take(*rring.keys(step))
    if far:
        @pl.loop(0, far)
        def _(i):
            at = lax.rem(2 * y + nd // 2 + i, nd)
            split_slot(at)
            slot(at)

    local[6].wait()

    def finish(at):
        update = jnp.concatenate([ubuf[i, at, 0:rows] for i in range(nd)], axis=1)
        tbuf[at, :] = tbuf[at, :] - update

    step = 32
    if rows >= step:
        @pl.loop(0, rows // step)
        def _(i):
            finish(tile(i, step))

    finish(slice(rows // step * step, rows))
    t_copy = pltpu.make_async_copy(tbuf, t_out, load.at[2])
    t_copy.start()

    trade.wait_send()
    for each in (ysmall, xsmall, zsmall, rring, zbulk, xbulk, lbulk, rrelay, zrelay, xrelay):
        each.drain()
    for c in range(2):
        lsmall_sends(c, lambda copy: copy.wait_send())

    @pl.when(on_edge)
    def _():
        for c in range(2):
            for j in range(1, nz):
                zscatter(c, j).wait_send()

    @pl.when(root)
    def _():
        for c in range(2):
            for i in range(1, nx):
                lscatter(c, i).wait_send()

    c_copy.wait()
    p_copy.wait()
    t_copy.wait()


def body(dims, trailing, panel_block, factor_panel, corner_block, corner_inverse):
    nx, nz, ny = dims
    nd = 2 * ny
    rows, width = panel_block.shape
    pad = max(-(-rows // (8 * nx)) * 8 * nx, -(-rows // 16) * 16)
    corner_rows = corner_block.shape[0]
    vmem = pltpu.VMEM
    square = vmem((width, width), BF16)
    any_space = pl.BlockSpec(memory_space=pl.ANY)

    def sems(*counts):
        return [pltpu.SemaphoreType.DMA((n,)) for n in counts for _ in range(2)]

    scratch = [
        vmem((nd, 2, rows, width), F32),
        vmem((nd, 2, pad, width), BF16), vmem((nd, 2, pad, width), BF16),
        vmem((2, pad, width), F32), vmem((2, pad, width), F32),
        vmem((2, 2 * pad, width), BF16), vmem((2, 2 * pad, width), BF16),
        vmem((2, nx, nz, 8 * ny, width), F32),
        vmem((2, corner_rows, width), F32), vmem((corner_rows, width), F32),
        *[square] * 8,
        vmem((2, pad, width), BF16), vmem((2, pad, width), BF16),
        vmem((rows, width), F32),
        vmem((nd, pad, 256), F32),
        vmem(trailing.shape, F32),
        vmem((corner_rows, width), F32),
        pltpu.SemaphoreType.DMA((7,)),
        *sems(ny, 4 * ny, nx, nz, 4 * nz, 4 * nx, 2 * nz, 4 * nx, 4 * ny + 4, 4 * nz + 4, 4 * nx + 4),
        pltpu.SemaphoreType.DMA, pltpu.SemaphoreType.DMA,
        *sems(2 * nx, 2 * nz),
    ]
    return pl.pallas_call(
        functools.partial(kernel, dims),
        out_shape=(
            jax.ShapeDtypeStruct(trailing.shape, F32),
            jax.ShapeDtypeStruct(panel_block.shape, F32),
            jax.ShapeDtypeStruct(corner_block.shape, F32),
        ),
        in_specs=[any_space] * 5,
        out_specs=(any_space,) * 3,
        scratch_shapes=scratch,
        compiler_params=pltpu.CompilerParams(
            collective_id=0, has_side_effects=True, vmem_limit_bytes=67_000_000
        ),
        name="panel_step",
    )(trailing, panel_block, factor_panel, corner_block, corner_inverse)


def solution(mesh):
    dims = (mesh.shape["row"], mesh.shape["col"], mesh.shape["depth"] // 2)
    columns = P("depth", ("row", "col"))
    spread = P(("row", "col", "depth"), None)
    return jax.shard_map(
        functools.partial(body, dims),
        mesh=mesh,
        in_specs=(columns, spread, spread, spread, spread),
        out_specs=(columns, spread, spread),
        check_vma=False,
    )
```
